512 devices in a mesh: grp: 4 (over y), row: 128 (over x, z, core).
Axes of the slice: x: 4, y: 4, z: 16, core: 2. Of those that a mesh axis runs over, the one named last changes fastest.
Arguments:
- a_tiles: bfloat16 [1024, 4, 7, 128, 128], P('row', 'grp'), may hold values from -0.5 to 0.5
- a_cols: int32 [1024, 4, 7], P('row', 'grp'), may hold values from 0 to 1023, as said below
- p_tiles: bfloat16 [1024, 4, 128, 128], P('row'), may hold values from -0.5 to 0.5
- p_cols: int32 [1024, 4], replicated, may hold values from 0 to 511, as said below
- c_cols: int32 [512, 16], replicated, may hold values from 0 to 511, as said below
Outputs:
- coarse: float32 [512, 16, 128, 128], P('row', 'grp')
The draws below stay inside these ranges and needn't reach their ends.
Inputs may be any that keep to these rules, and one draw needn't show every extreme that they name: For fine tile row i in block b = i // 8, every entry of a_cols[i] lies in [max(b - 2, 0) * 8, min(b + 3, 128) * 8). For fine tile row i in block b = i // 8, the entries of p_cols[i] are distinct and lie in [(b - 1) * 4, (b + 2) * 4). For coarse tile row c in block t = c // 4, the entries of c_cols[c] are distinct and lie among the 20 coarse tile rows that start at min(max(t - 2, 0), 123) * 4.
All inputs are finite; a program needn't handle non-finite values.
Results may differ from the reference program's by a relative error of at most 0.0003.
Values may be sent and summed in bfloat16 or wider, within the bound.
A program may use at most 128 MiB of HBM per device.

```python
import jax
import jax.numpy as jnp
from jax import lax

TILE = 128
CT_DEV = 4
SLOTS = 7
KP = 4
KC = 16
FT_DEV = 8
GROUPS = 4
FT = 1024
NCT = 512


def pick_distinct(key, count, width, valid, take):
    offsets = jnp.arange(width, dtype=jnp.int32)[None, :]
    scores = jax.random.randint(key, (count, width), 0, 1 << 20, dtype=jnp.int32) * width + offsets
    scores = jnp.where(valid, scores, -1 - offsets)
    top_scores, chosen = lax.top_k(scores, take)
    return chosen.astype(jnp.int32)


def draw_a_cols(key, part):
    fine_ids = jnp.arange(FT, dtype=jnp.int32)
    owner = fine_ids // FT_DEV
    lowest = jnp.maximum(owner - 2, 0) * FT_DEV
    highest_row = jnp.minimum(owner + 3, FT // FT_DEV) * FT_DEV
    spans = (highest_row - lowest)[:, None, None]
    picks = jax.random.randint(jax.random.fold_in(key, 17), (FT, GROUPS, SLOTS), 0, 1 << 30, dtype=jnp.int32)
    return (lowest[:, None, None] + picks % spans).astype(jnp.int32)


def draw_p_cols(key, part):
    fine_ids = jnp.arange(FT, dtype=jnp.int32)
    owner = fine_ids // FT_DEV
    begin = (owner - 1) * CT_DEV
    candidate = begin[:, None] + jnp.arange(3 * CT_DEV, dtype=jnp.int32)[None, :]
    valid = (candidate >= 0) & (candidate < NCT)
    chosen = pick_distinct(jax.random.fold_in(key, 29), FT, 3 * CT_DEV, valid, KP)
    return (begin[:, None] + chosen).astype(jnp.int32)


def draw_c_cols(key, part):
    coarse_ids = jnp.arange(NCT, dtype=jnp.int32)
    owner = coarse_ids // CT_DEV
    begin = jnp.clip(owner - 2, 0, NCT // CT_DEV - 5) * CT_DEV
    valid = jnp.ones((NCT, 5 * CT_DEV), dtype=bool)
    chosen = pick_distinct(jax.random.fold_in(key, 41), NCT, 5 * CT_DEV, valid, KC)
    return (begin[:, None] + chosen).astype(jnp.int32)


def block_levels(own_key, dims, pieces, least, high):
    gain = 1.0
    for axis_at, blocks in pieces:
        draws = jax.random.uniform(jax.random.fold_in(jax.random.fold_in(own_key, 6), axis_at), (blocks,), jnp.float32, least / len(pieces), high / len(pieces))
        gain = gain * jnp.repeat(jnp.exp(draws), dims[axis_at] // blocks).reshape((-1,) + (1,) * (len(dims) - 1 - axis_at))
    return gain


def normal_values(rng, dims, scale, bound, split=(), kind=jnp.bfloat16):
    loudness = block_levels(rng, dims, split, -0.22, 0.18) if split else 1.0
    entries = jax.random.normal(rng, dims, jnp.float32) * scale * loudness
    return jnp.minimum(jnp.maximum(entries, -bound), bound).astype(kind)


def setup_inputs(seed: int = 0) -> dict:
    splits = jax.random.split(jax.random.key(seed), 6)
    a_tiles = normal_values(splits[0], (FT, GROUPS, SLOTS, TILE, TILE), TILE ** -0.5, 0.5, ((0, 128), (1, 4)))
    a_cols = draw_a_cols(jax.random.fold_in(splits[5], 71), 0)
    p_tiles = normal_values(splits[2], (FT, KP, TILE, TILE), TILE ** -0.5, 0.5, ((0, 128),))
    p_cols = draw_p_cols(jax.random.fold_in(splits[5], 71), 0)
    c_cols = draw_c_cols(jax.random.fold_in(splits[5], 71), 0)
    return dict(a_tiles=a_tiles, a_cols=a_cols, p_tiles=p_tiles, p_cols=p_cols, c_cols=c_cols)


highest = lax.Precision.HIGHEST


def reference(a_tiles, a_cols, p_tiles, p_cols, c_cols):
    def fine_row(coarse, inputs):
        a_row, columns, own_tiles, own_cols = inputs
        targets = c_cols[own_cols]
        fetched = p_tiles[columns].astype(jnp.float32)
        fetched_cols = p_cols[columns]
        products = jnp.einsum("gsxy,gspyz->gspxz", a_row.astype(jnp.float32), fetched, precision=highest)
        matches = (fetched_cols[:, :, :, None, None] == targets[None, None, None, :, :]).astype(jnp.float32)
        partial_value = jnp.einsum("gspxz,gspqk->gqkxz", products, matches, precision=highest)
        summed = jnp.sum(partial_value, axis=0)
        row_terms = jnp.einsum("qyx,qkyz->qkxz", own_tiles.astype(jnp.float32), summed, precision=highest)
        return coarse.at[own_cols].add(row_terms), None

    initial = jnp.zeros((NCT, KC, TILE, TILE), jnp.float32)
    result = lax.scan(fine_row, initial, (a_tiles, a_cols, p_tiles, p_cols))[0]
    return result
```

```python
import jax
import jax.numpy as jnp
from jax import lax
from jax.experimental import pallas as pl
from jax.experimental.pallas import tpu as pltpu
from jax.sharding import PartitionSpec as P

MESH = pl.DeviceIdType.MESH
F32 = jnp.float32
BF16 = jnp.bfloat16
STEPS = (2, 1, 3, 0)


def index_table(a_cols, p_cols, c_cols):
    rows, cols = 8, 4
    position = lax.axis_index("row")
    first = position * rows
    base = (position - 3) * cols
    padded = jnp.pad(p_cols, ((2 * rows, 2 * rows), (0, 0)), constant_values=-1000)
    band = lax.dynamic_slice_in_dim(padded, first, 5 * rows, 0) - base
    tile = jnp.arange(4, dtype=jnp.int32)
    window = jnp.arange(28, dtype=jnp.int32)
    place = jnp.where(band[:, :, None] == window, tile[None, :, None], 4).min(axis=1)
    own = lax.dynamic_slice_in_dim(p_cols, first, rows, 0) - (position - 1) * cols
    coarse = jnp.arange(12, dtype=jnp.int32)
    which = jnp.where(own[:, :, None] == coarse, tile[None, :, None], 4).min(axis=1).T
    padded_c = jnp.pad(c_cols, ((cols, cols), (0, 0)))
    target = lax.dynamic_slice_in_dim(padded_c, position * cols, 12, 0) - base
    target = jnp.where((target >= 0) & (target < 28), target, 28)
    local = a_cols[:, 0, :] - (first - 2 * rows)

    def wide(x):
        return jnp.pad(x, ((0, 0), (0, 128 - x.shape[1])))

    return jnp.concatenate([wide(place), wide(local), wide(target), wide(which)], axis=0), wide(local)


def kernel(
    tab, cols_hbm, a_hbm, p_hbm, out_hbm,
    a_own, a_far, p_own, p_turn, band, spreadable, placed, window, lower, upper,
    from_next, from_prev, center, gathered, out_v, cols_v, cols_s,
    load_sem, a_send, a_recv, c_send, c_recv, p_send, p_recv, s_send, s_recv, g_send, g_recv, out_sem,
):
    grp = lax.axis_index("grp")
    row = lax.axis_index("row")
    n_row = lax.axis_size("row")
    core = lax.rem(row, 2)
    half = lax.rem(grp, 2)

    def along_row(by):
        return (grp, lax.rem(row + by + n_row, n_row))

    def along_grp(by):
        return (lax.rem(grp + by, 4), row)

    partner = (jnp.where(core == 0, grp + 1 - 2 * half, 3 - grp), row)
    sibling = (grp, row + 1 - 2 * core)

    load_p = pltpu.make_async_copy(p_hbm, p_own, load_sem.at[0])
    load_p.start()
    load_a = pltpu.make_async_copy(a_hbm, a_own, load_sem.at[1])
    load_a.start()

    barrier = pltpu.get_barrier_semaphore()
    peers = [along_grp(1), along_grp(2), along_grp(3)] + [along_row(by) for by in (1, -1, 2, -2)]
    for peer in peers:
        pl.semaphore_signal(barrier, inc=1, device_id=peer, device_id_type=MESH)
    pl.semaphore_wait(barrier, len(peers))

    def remote(src, dst, send, recv, device):
        return pltpu.make_async_remote_copy(
            src_ref=src, dst_ref=dst, send_sem=send, recv_sem=recv, device_id=device, device_id_type=MESH
        )

    def a_copy(i):
        return remote(a_hbm.at[i], a_far.at[i], a_send.at[i], a_recv.at[i], partner)

    cols_copy = remote(cols_hbm, cols_v, c_send, c_recv, partner)
    cols_copy.start()
    for i in range(8):
        a_copy(i).start()

    left = lax.broadcasted_iota(jnp.int32, (128, 128), 1) < 64

    def turn(x):
        return pltpu.roll(x.astype(F32), 64, 1).astype(x.dtype)

    load_p.wait()

    def halve(i, carry):
        for pair in range(2):
            x, y = p_own[i, 2 * pair], p_own[i, 2 * pair + 1]
            x_turned, y_turned = turn(x), turn(y)
            first = jnp.where(left, x, y_turned)
            second = jnp.where(left, x_turned, y)
            band[2, i, pair] = jnp.where(half == 0, first, second)
        return carry

    lax.fori_loop(0, 8, halve, 0)

    def transpose(i, carry):
        for q in range(4):
            p_turn[i, q] = p_own[i, q].T
        p_turn[i, 4] = jnp.zeros((128, 128), BF16)
        return carry

    lax.fori_loop(0, 8, transpose, 0)

    up_slot = 3 - 2 * core
    there = 1 + 2 * core
    forward_slot = 4 - 4 * core
    p_next = remote(band.at[2], band.at[0], p_send.at[0], p_recv.at[0], along_row(2))
    p_prev = remote(band.at[2], band.at[4], p_send.at[1], p_recv.at[4], along_row(-2))
    p_sib = remote(band.at[2], band.at[there], p_send.at[2], p_recv.at[there], sibling)
    p_fwd = remote(band.at[forward_slot], band.at[up_slot], p_send.at[3], p_recv.at[up_slot], sibling)
    p_next.start()
    p_prev.start()
    p_sib.start()

    spreadable[4] = jnp.zeros((128, 128), BF16)

    def place_block(slot):
        def place(n, carry):
            line = slot * 8 + n
            for pair in range(2):
                x = band[slot, n, pair]
                turned = turn(x)
                spreadable[2 * pair] = jnp.where(left, x, turned)
                spreadable[2 * pair + 1] = jnp.where(left, turned, x)
            for w in range(14):
                first = spreadable[tab[line, 2 * w]]
                second = spreadable[tab[line, 2 * w + 1]]
                placed[line, w // 2, :, (w % 2) * 128 : (w % 2 + 1) * 128] = jnp.where(left, first, second)
            return carry

        lax.fori_loop(0, 8, place, 0)

    def arrived(slot):
        remote(band.at[slot], band.at[slot], p_send.at[0], p_recv.at[slot], sibling).wait_recv()

    place_block(2)
    arrived(up_slot)
    place_block(up_slot)
    arrived(forward_slot)
    p_fwd.start()
    place_block(forward_slot)
    arrived(4 - forward_slot)
    place_block(4 - forward_slot)
    arrived(4 - up_slot)
    place_block(4 - up_slot)

    cols_copy.wait_recv()
    to_smem = pltpu.make_async_copy(cols_v, cols_s, load_sem.at[2])
    to_smem.start()
    to_smem.wait()
    load_a.wait()

    def fine_row(i, carry):
        window[i, 28] = jnp.zeros((128, 128), BF16)
        a_copy(i).wait_recv()
        lhs = jnp.concatenate([a_own[i, s] for s in range(7)] + [a_far[i, s] for s in range(7)], axis=1)
        lines = [tab[40 + i, s] for s in range(7)] + [cols_s[i, s] for s in range(7)]
        for n in range(7):
            rhs = jnp.concatenate([placed[line, n] for line in lines], axis=0)
            acc = jnp.dot(lhs, rhs, preferred_element_type=F32)
            for u in range(2):
                value = acc[:, u * 128 : (u + 1) * 128]
                high = value.astype(BF16).astype(F32)
                low = value - high
                window[i, 4 * n + 2 * u] = jnp.where(left, high, pltpu.roll(low, 64, 1)).astype(BF16)
                window[i, 4 * n + 2 * u + 1] = jnp.where(left, pltpu.roll(high, 64, 1), low).astype(BF16)
        return carry

    lax.fori_loop(0, 8, fine_row, 0)

    def quarter(t):
        step = jnp.where(t == 0, STEPS[0], jnp.where(t == 1, STEPS[1], jnp.where(t == 2, STEPS[2], STEPS[3])))
        return lax.rem(grp + step, 4)

    def coarse_tiles(c, t):
        lhs = jnp.concatenate([p_turn[i, tab[60 + c, i]] for i in range(8)], axis=1)
        k = quarter(t) * 4
        tiles = []
        for pair in range(2):
            first = tab[48 + c, k + 2 * pair]
            second = tab[48 + c, k + 2 * pair + 1]
            rhs = jnp.concatenate(
                [jnp.concatenate([window[i, first], window[i, second]], axis=1) for i in range(8)], axis=0
            )
            acc = jnp.dot(lhs, rhs, preferred_element_type=F32)
            x, y = acc[:, :128], acc[:, 128:]
            tiles.append(jnp.where(left, x, y) + pltpu.roll(jnp.where(left, y, x), 64, 1))
        return tiles

    def lower_copy(c, t):
        return remote(lower.at[c, t], from_next.at[c, t], s_send.at[0, c, t], s_recv.at[0, c, t], along_row(-1))

    def upper_copy(c, t):
        return remote(upper.at[c, t], from_prev.at[c, t], s_send.at[1, c, t], s_recv.at[1, c, t], along_row(1))

    def sides(c):
        def one(t, carry):
            for pair, tile in enumerate(coarse_tiles(c, t)):
                lower[c, t, pair] = tile
            for pair, tile in enumerate(coarse_tiles(8 + c, t)):
                upper[c, t, pair] = tile

            @pl.when(t > 0)
            def _():
                lower_copy(c, t - 1).start()
                upper_copy(c, t - 1).start()

            return carry

        lax.fori_loop(0, 4, one, 0)
        lower_copy(c, 3).start()
        upper_copy(c, 3).start()

    def middle(c):
        def one(t, carry):
            for pair, tile in enumerate(coarse_tiles(4 + c, t)):
                center[c, t, pair] = tile
            return carry

        lax.fori_loop(0, 4, one, 0)

    def group_copy(c, t):
        return remote(
            center.at[c, t], gathered.at[t, c], g_send.at[t, c], g_recv.at[t, c], along_grp(STEPS[t])
        )

    def absorb(c):
        for t in range(4):
            lower_copy(c, t).wait_recv()
            upper_copy(c, t).wait_recv()
            center[c, t] = center[c, t] + (from_next[c, t] + from_prev[c, t])
            if t > 0:
                group_copy(c, t - 1).start()

    def out_copy(c):
        return pltpu.make_async_copy(out_v.at[c], out_hbm.at[c], out_sem.at[c])

    def finish(c):
        for t in range(3):
            group_copy(c, t).wait_recv()
        for pair in range(2):
            same = center[c, 3, pair] + gathered[0, c, pair]
            other = gathered[1, c, pair] + gathered[2, c, pair]
            x = jnp.where(half == 0, same, other)
            y = jnp.where(half == 0, other, same)
            out_v[c, 2 * pair] = jnp.where(left, x, pltpu.roll(y, 64, 1))
            out_v[c, 2 * pair + 1] = jnp.where(left, pltpu.roll(x, 64, 1), y)
        out_copy(c).start()

    sides(0)
    middle(0)
    sides(1)
    absorb(0)
    middle(1)
    sides(2)
    absorb(1)
    middle(2)
    sides(3)
    absorb(2)
    middle(3)
    absorb(3)
    for c in range(4):
        finish(c)

    cols_copy.wait_send()
    for i in range(8):
        a_copy(i).wait_send()
    p_next.wait_send()
    p_prev.wait_send()
    p_sib.wait_send()
    p_fwd.wait_send()
    for c in range(4):
        for t in range(4):
            lower_copy(c, t).wait_send()
            upper_copy(c, t).wait_send()
        for t in range(3):
            group_copy(c, t).wait_send()
        out_copy(c).wait()


def body(a_tiles, a_cols, p_tiles, p_cols, c_cols):
    table, local = index_table(a_cols, p_cols, c_cols)
    dma = pltpu.SemaphoreType.DMA
    anywhere = pl.BlockSpec(memory_space=pl.ANY)
    return pl.pallas_call(
        kernel,
        out_shape=jax.ShapeDtypeStruct((4, 4, 128, 128), F32),
        in_specs=[pl.BlockSpec(memory_space=pltpu.SMEM), anywhere, anywhere, anywhere],
        out_specs=anywhere,
        scratch_shapes=[
            pltpu.VMEM((8, 7, 128, 128), BF16),
            pltpu.VMEM((8, 7, 128, 128), BF16),
            pltpu.VMEM((8, 4, 128, 128), BF16),
            pltpu.VMEM((8, 5, 128, 128), BF16),
            pltpu.VMEM((5, 8, 2, 128, 128), BF16),
            pltpu.VMEM((5, 128, 128), BF16),
            pltpu.VMEM((40, 7, 128, 256), BF16),
            pltpu.VMEM((8, 29, 128, 128), BF16),
            pltpu.VMEM((4, 4, 2, 128, 128), F32),
            pltpu.VMEM((4, 4, 2, 128, 128), F32),
            pltpu.VMEM((4, 4, 2, 128, 128), F32),
            pltpu.VMEM((4, 4, 2, 128, 128), F32),
            pltpu.VMEM((4, 4, 2, 128, 128), F32),
            pltpu.VMEM((3, 4, 2, 128, 128), F32),
            pltpu.VMEM((4, 4, 128, 128), F32),
            pltpu.VMEM((8, 128), jnp.int32),
            pltpu.SMEM((8, 128), jnp.int32),
            dma((3,)),
            dma((8,)),
            dma((8,)),
            dma,
            dma,
            dma((4,)),
            dma((5,)),
            dma((2, 4, 4)),
            dma((2, 4, 4)),
            dma((3, 4)),
            dma((3, 4)),
            dma((4,)),
        ],
        compiler_params=pltpu.CompilerParams(
            collective_id=0, has_side_effects=True, vmem_limit_bytes=60 * 1024 * 1024
        ),
        cost_estimate=pl.CostEstimate(flops=4_000_000_000, bytes_accessed=8_000_000, transcendentals=0),
    )(table, local, a_tiles.reshape(8, 7, 128, 128), p_tiles)


def solution(mesh):
    return jax.shard_map(
        body,
        mesh=mesh,
        in_specs=(
            P("row", "grp", None, None, None),
            P("row", "grp", None),
            P("row", None, None, None),
            P(),
            P(),
        ),
        out_specs=P("row", "grp", None, None),
        check_vma=False,
    )
```

```python
import jax
import jax.numpy as jnp
from jax import lax
from jax.experimental import pallas as pl
from jax.experimental.pallas import tpu as pltpu
from jax.sharding import PartitionSpec as P

MESH = pl.DeviceIdType.MESH
F32 = jnp.float32
BF16 = jnp.bfloat16
I32 = jnp.int32
PLACE, WHICH, TARGET = 0, 32, 48
BEHIND = 4


def kernel(
    a_cols_hbm, p_cols_hbm, c_cols_hbm, a_hbm, p_hbm, out_v,
    a_own, a_far, p_own, p_turn, band, spreadable, placed, window, outer, inner,
    from_outer, from_inner, center, gathered, p_cols_v, c_cols_v, far_cols_v, tab_v, tab, own_cols, far_cols,
    load_sem, a_send, a_recv, c_send, c_recv, p_send, p_recv, s_send, s_recv, g_send, g_recv,
):
    grp = lax.axis_index("grp")
    row = lax.axis_index("row")
    n_row = lax.axis_size("row")
    core = lax.rem(row, 2)
    half = lax.rem(grp, 2)

    def along_row(by):
        return (grp, lax.rem(row + by + n_row, n_row))

    def along_grp(by):
        return (lax.rem(grp + by, 4), row)

    partner = (jnp.where(core == 0, grp + 1 - 2 * half, 3 - grp), row)
    sibling = (grp, row + 1 - 2 * core)
    outside = along_row(2 * core - 1)

    def remote(src, dst, send, recv, device):
        return pltpu.make_async_remote_copy(
            src_ref=src, dst_ref=dst, send_sem=send, recv_sem=recv, device_id=device, device_id_type=MESH
        )

    load_p = pltpu.make_async_copy(p_hbm, p_own, load_sem.at[0])
    load_p_cols = pltpu.make_async_copy(p_cols_hbm, p_cols_v.at[:, pl.ds(128, 1024)], load_sem.at[1])
    load_c_cols = pltpu.make_async_copy(c_cols_hbm, c_cols_v.at[:, pl.ds(128, 512)], load_sem.at[2])
    load_a = pltpu.make_async_copy(a_hbm, a_own, load_sem.at[3])
    load_own_cols = pltpu.make_async_copy(a_cols_hbm, own_cols, load_sem.at[4])
    for load in (load_p, load_p_cols, load_c_cols, load_a, load_own_cols):
        load.start()

    barrier = pltpu.get_barrier_semaphore()
    peers = [along_grp(1), along_grp(2), along_grp(3)] + [along_row(by) for by in (1, -1, 2, -2)]
    for peer in peers:
        pl.semaphore_signal(barrier, inc=1, device_id=peer, device_id_type=MESH)

    lane = lax.broadcasted_iota(I32, (1, 128), 1)

    def from_lane(ref, start):
        begin = start + 128
        tile = begin // 128
        shift = lax.rem(begin, 128)
        first = pltpu.roll(ref[:, pl.ds(pl.multiple_of(tile * 128, 128), 128)], 128 - shift, 1)
        second = pltpu.roll(ref[:, pl.ds(pl.multiple_of(tile * 128 + 128, 128), 128)], 128 - shift, 1)
        return jnp.where(lane < 128 - shift, first, second)

    load_p_cols.wait()
    load_c_cols.wait()
    band_cols = from_lane(p_cols_v, row * 8 - 16)
    sub = lax.broadcasted_iota(I32, (32, 128), 0)
    place = jnp.full((32, 128), 4, I32)
    which = jnp.full((16, 128), 4, I32)
    for p in range(4):
        cols = band_cols[p : p + 1]
        place = jnp.where(cols - (row - 3) * 4 == sub, p, place)
        which = jnp.where(cols - (row - 1) * 4 == sub[:16], p, which)
    target = from_lane(c_cols_v, row * 4 - 4) - (row - 3) * 4
    tab_v[PLACE : PLACE + 32] = place
    tab_v[WHICH : WHICH + 16] = which
    tab_v[TARGET : TARGET + 16] = jnp.where((target >= 0) & (target < 28), target, 28)

    left = lax.broadcasted_iota(I32, (128, 128), 1) < 64

    def turn(x):
        return pltpu.roll(x.astype(F32), 64, 1).astype(x.dtype)

    load_p.wait()

    def halve(i, carry):
        for pair in range(2):
            x, y = p_own[i, 2 * pair], p_own[i, 2 * pair + 1]
            x_turned, y_turned = turn(x), turn(y)
            first = jnp.where(left, x, y_turned)
            second = jnp.where(left, x_turned, y)
            band[2, i, pair] = jnp.where(half == 0, first, second)
        return carry

    lax.fori_loop(0, 8, halve, 0)

    pl.semaphore_wait(barrier, len(peers))

    def a_copy(i):
        return remote(a_hbm.at[i], a_far.at[i], a_send.at[i], a_recv.at[i], partner)

    cols_copy = remote(a_cols_hbm, far_cols_v, c_send, c_recv, partner)
    cols_copy.start()
    for i in range(8):
        a_copy(i).start()

    sibling_slot = 3 - 2 * core
    there = 1 + 2 * core
    pass_slot = 4 - 4 * core
    other_slot = 4 * core
    passed_slot = 4 - sibling_slot

    def p_copy(kind, src, dst, n, device):
        lines = pl.ds(2 * n, 2)
        return remote(band.at[src, lines], band.at[dst, lines], p_send.at[kind, n], p_recv.at[dst, n], device)

    def p_next(n):
        return p_copy(0, 2, 0, n, along_row(2))

    def p_prev(n):
        return p_copy(1, 2, 4, n, along_row(-2))

    def p_sibling(n):
        return p_copy(2, 2, there, n, sibling)

    def p_pass(n):
        return p_copy(3, pass_slot, sibling_slot, n, sibling)

    for n in range(4):
        p_next(n).start()
        p_prev(n).start()
    for n in range(4):
        p_sibling(n).start()

    to_smem = pltpu.make_async_copy(tab_v, tab, load_sem.at[5])
    to_smem.start()

    def transpose(i, carry):
        for q in range(4):
            p_turn[i, q] = p_own[i, q].T
        p_turn[i, 4] = jnp.zeros((128, 128), BF16)
        window[i, 28] = jnp.zeros((128, 128), BF16)
        return carry

    lax.fori_loop(0, 8, transpose, 0)
    spreadable[4] = jnp.zeros((128, 128), BF16)
    to_smem.wait()

    def place_lines(slot, begin, count):
        def one(n, carry):
            line = slot * 8 + n
            for pair in range(2):
                x = band[slot, n, pair]
                turned = turn(x)
                spreadable[2 * pair] = jnp.where(left, x, turned)
                spreadable[2 * pair + 1] = jnp.where(left, turned, x)
            for w in range(14):
                first = spreadable[tab[PLACE + 2 * w, line]]
                second = spreadable[tab[PLACE + 2 * w + 1, line]]
                placed[line, w // 2, :, (w % 2) * 128 : (w % 2 + 1) * 128] = jnp.where(left, first, second)
            return carry

        lax.fori_loop(begin, begin + count, one, 0)

    def arrived(slot, n):
        p_copy(0, slot, slot, n, sibling).wait_recv()

    place_lines(2, 0, 8)
    for n in range(4):
        arrived(sibling_slot, n)
    place_lines(sibling_slot, 0, 8)

    def place_chunk(n, carry):
        arrived(pass_slot, n)
        p_pass(n).start()
        place_lines(pass_slot, 2 * n, 2)
        arrived(other_slot, n)
        place_lines(other_slot, 2 * n, 2)
        arrived(passed_slot, n)
        place_lines(passed_slot, 2 * n, 2)
        return carry

    lax.fori_loop(0, 4, place_chunk, 0)

    cols_copy.wait_recv()
    far_to_smem = pltpu.make_async_copy(far_cols_v, far_cols, load_sem.at[6])
    far_to_smem.start()
    load_own_cols.wait()
    load_a.wait()
    far_to_smem.wait()
    first_line = row * 8 - 16

    def fine_row(i, carry):
        a_copy(i).wait_recv()
        lhs = jnp.concatenate([a_own[i, s] for s in range(7)] + [a_far[i, s] for s in range(7)], axis=1)
        lines = [ref[s, 0, i] - first_line for ref in (own_cols, far_cols) for s in range(7)]
        lines = [jnp.clip(line, 0, 39) for line in lines]
        for n in range(7):
            rhs = jnp.concatenate([placed[line, n] for line in lines], axis=0)
            acc = jnp.dot(lhs, rhs, preferred_element_type=F32)
            for u in range(2):
                value = acc[:, u * 128 : (u + 1) * 128]
                high = value.astype(BF16).astype(F32)
                low = value - high
                window[i, 4 * n + 2 * u] = jnp.where(left, high, pltpu.roll(low, 64, 1)).astype(BF16)
                window[i, 4 * n + 2 * u + 1] = jnp.where(left, pltpu.roll(high, 64, 1), low).astype(BF16)
        return carry

    lax.fori_loop(0, 8, fine_row, 0)

    def unit(n):
        early = n < 12
        return jnp.where(early, n // 3, n - 12), jnp.where(early, lax.rem(n, 3), 3)

    def steps(t):
        return jnp.where(t == 0, 2, jnp.where(t == 1, 1, jnp.where(t == 2, 3, 0)))

    def coarse_tiles(c, t):
        lhs = jnp.concatenate([p_turn[i, tab[WHICH + c, 16 + i]] for i in range(8)], axis=1)
        k = TARGET + lax.rem(grp + steps(t), 4) * 4
        tiles = []
        for pair in range(2):
            first = tab[k + 2 * pair, c]
            second = tab[k + 2 * pair + 1, c]
            rhs = jnp.concatenate(
                [jnp.concatenate([window[i, first], window[i, second]], axis=1) for i in range(8)], axis=0
            )
            acc = jnp.dot(lhs, rhs, preferred_element_type=F32)
            x, y = acc[:, :128], acc[:, 128:]
            tiles.append(jnp.where(left, x, y) + pltpu.roll(jnp.where(left, y, x), 64, 1))
        return tiles

    def outer_copy(n):
        return remote(outer.at[n], from_outer.at[n], s_send.at[0, n], s_recv.at[0, n], outside)

    def inner_copy(n):
        return remote(inner.at[n], from_inner.at[n], s_send.at[1, n], s_recv.at[1, n], sibling)

    def group_copy(c, t):
        return remote(
            center.at[3 * c + t], gathered.at[t, c], g_send.at[t, c], g_recv.at[t, c], along_grp(steps(t))
        )

    def fill(ref, n, c, t):
        for pair, tile in enumerate(coarse_tiles(c, t)):
            ref[n, pair] = tile

    def absorb(n):
        outer_copy(n).wait_recv()
        inner_copy(n).wait_recv()
        center[n] = center[n] + (from_outer[n] + from_inner[n])

    def one_unit(n, carry):
        c, t = unit(n)

        @pl.when(n >= BEHIND)
        def _():
            absorb(n - BEHIND)

        fill(outer, n, c + 8 * core, t)

        @pl.when(n >= BEHIND)
        def _():
            done_c, done_t = unit(n - BEHIND)
            group_copy(done_c, done_t).start()

        fill(inner, n, c + 8 - 8 * core, t)
        outer_copy(n).start()
        fill(center, n, c + 4, t)
        inner_copy(n).start()
        return carry

    lax.fori_loop(0, 16, one_unit, 0)

    for c in range(4):
        absorb(12 + c)
        for t in range(3):
            group_copy(c, t).wait_recv()
        for pair in range(2):
            same = center[12 + c, pair] + gathered[0, c, pair]
            other = gathered[1, c, pair] + gathered[2, c, pair]
            x = jnp.where(half == 0, same, other)
            y = jnp.where(half == 0, other, same)
            out_v[c, 2 * pair] = jnp.where(left, x, pltpu.roll(y, 64, 1))
            out_v[c, 2 * pair + 1] = jnp.where(left, pltpu.roll(x, 64, 1), y)

    cols_copy.wait_send()
    for i in range(8):
        a_copy(i).wait_send()
    for n in range(4):
        for copy in (p_next(n), p_prev(n), p_sibling(n), p_pass(n)):
            copy.wait_send()

    def sent(n, carry):
        outer_copy(n).wait_send()
        inner_copy(n).wait_send()

        @pl.when(n < 12)
        def _():
            group_copy(n // 3, lax.rem(n, 3)).wait_send()

        return carry

    lax.fori_loop(0, 16, sent, 0)


def body(a_tiles, a_cols, p_tiles, p_cols, c_cols):
    dma = pltpu.SemaphoreType.DMA
    anywhere = pl.BlockSpec(memory_space=pl.ANY)
    side = pltpu.VMEM((16, 2, 128, 128), F32)
    return pl.pallas_call(
        kernel,
        out_shape=jax.ShapeDtypeStruct((4, 4, 128, 128), F32),
        in_specs=[anywhere] * 5,
        out_specs=pl.BlockSpec(memory_space=pltpu.VMEM),
        scratch_shapes=[
            pltpu.VMEM((8, 7, 128, 128), BF16),
            pltpu.VMEM((8, 7, 128, 128), BF16),
            pltpu.VMEM((8, 4, 128, 128), BF16),
            pltpu.VMEM((8, 5, 128, 128), BF16),
            pltpu.VMEM((5, 8, 2, 128, 128), BF16),
            pltpu.VMEM((5, 128, 128), BF16),
            pltpu.VMEM((40, 7, 128, 256), BF16),
            pltpu.VMEM((8, 29, 128, 128), BF16),
            side,
            side,
            side,
            side,
            side,
            pltpu.VMEM((3, 4, 2, 128, 128), F32),
            pltpu.VMEM((4, 1280), I32),
            pltpu.VMEM((16, 768), I32),
            pltpu.VMEM((7, 1, 8), I32),
            pltpu.VMEM((64, 128), I32),
            pltpu.SMEM((64, 128), I32),
            pltpu.SMEM((7, 1, 8), I32),
            pltpu.SMEM((7, 1, 8), I32),
            dma((7,)),
            dma((8,)),
            dma((8,)),
            dma,
            dma,
            dma((4, 4)),
            dma((5, 4)),
            dma((2, 16)),
            dma((2, 16)),
            dma((3, 4)),
            dma((3, 4)),
        ],
        compiler_params=pltpu.CompilerParams(
            collective_id=0, has_side_effects=True, vmem_limit_bytes=52 * 1024 * 1024
        ),
        cost_estimate=pl.CostEstimate(flops=4_000_000_000, bytes_accessed=8_000_000, transcendentals=0),
    )(
        a_cols.transpose(2, 1, 0), p_cols.T, c_cols.T, a_tiles.reshape(8, 7, 128, 128), p_tiles
    )


def solution(mesh):
    return jax.shard_map(
        body,
        mesh=mesh,
        in_specs=(
            P("row", "grp", None, None, None),
            P("row", "grp", None),
            P("row", None, None, None),
            P(),
            P(),
        ),
        out_specs=P("row", "grp", None, None),
        check_vma=False,
    )
```

```python
import jax
import jax.numpy as jnp
from jax import lax
from jax.experimental import pallas as pl
from jax.experimental.pallas import tpu as pltpu
from jax.sharding import PartitionSpec as P

MESH = pl.DeviceIdType.MESH
F32 = jnp.float32
BF16 = jnp.bfloat16
I32 = jnp.int32
PLACE, WHICH, TARGET, PAIR, COLUMN = 0, 32, 48, 64, 80
BEHIND = 4
BEHIND_FIRST = 8


def kernel(
    a_cols_hbm, p_cols_hbm, c_cols_hbm, a_hbm, p_hbm, out_v,
    a_own, a_far, p_own, p_turn, band, spreadable, placed, window, outer, inner,
    from_outer, from_inner, center, gathered, p_cols_v, c_cols_v, far_cols_v, tab_v, tab, own_cols, far_cols,
    load_sem, a_send, a_recv, c_send, c_recv, p_send, p_recv, s_send, s_recv, g_send, g_recv, gate,
):
    grp = lax.axis_index("grp")
    row = lax.axis_index("row")
    n_row = lax.axis_size("row")
    core = lax.rem(row, 2)
    half = lax.rem(grp, 2)

    def along_row(by):
        return (grp, lax.rem(row + by + n_row, n_row))

    def along_grp(by):
        return (lax.rem(grp + by, 4), row)

    partner = (jnp.where(core == 0, grp + 1 - 2 * half, 3 - grp), row)
    sibling = (grp, row + 1 - 2 * core)
    outside = along_row(2 * core - 1)

    def remote(src, dst, send, recv, device):
        return pltpu.make_async_remote_copy(
            src_ref=src, dst_ref=dst, send_sem=send, recv_sem=recv, device_id=device, device_id_type=MESH
        )

    load_p = pltpu.make_async_copy(p_hbm, p_own, load_sem.at[0])
    load_p_cols = pltpu.make_async_copy(p_cols_hbm, p_cols_v.at[:, pl.ds(128, 1024)], load_sem.at[1])
    load_c_cols = pltpu.make_async_copy(c_cols_hbm, c_cols_v.at[:, pl.ds(128, 512)], load_sem.at[2])
    load_a = pltpu.make_async_copy(a_hbm, a_own, load_sem.at[3])
    load_own_cols = pltpu.make_async_copy(a_cols_hbm, own_cols, load_sem.at[4])
    for load in (load_p, load_p_cols, load_c_cols, load_a, load_own_cols):
        load.start()

    place_z = lax.rem(row // 2, 16)
    below = row >= 2
    above = row < n_row - 2
    first = (place_z == 0) & below
    last = (place_z == 15) & above
    has_outer = jnp.where(core == 0, row, n_row - 1 - row) >= 2

    barrier = pltpu.get_barrier_semaphore()

    def signal(semaphore, peer):
        pl.semaphore_signal(semaphore, inc=1, device_id=peer, device_id_type=MESH)

    for by in (1, 2, 3):
        signal(barrier, along_grp(by))
    signal(barrier, sibling)

    @pl.when(below)
    def _():
        signal(barrier, along_row(-2))

    @pl.when(below & (core == 0))
    def _():
        signal(barrier, along_row(-1))

    @pl.when(above & jnp.logical_not(last))
    def _():
        signal(barrier, along_row(2))

    @pl.when(above & jnp.logical_not(last) & (core == 1))
    def _():
        signal(barrier, along_row(1))


    lane = lax.broadcasted_iota(I32, (1, 128), 1)

    def from_lane(ref, start):
        begin = start + 128
        tile = begin // 128
        shift = lax.rem(begin, 128)
        first = pltpu.roll(ref[:, pl.ds(pl.multiple_of(tile * 128, 128), 128)], 128 - shift, 1)
        second = pltpu.roll(ref[:, pl.ds(pl.multiple_of(tile * 128 + 128, 128), 128)], 128 - shift, 1)
        return jnp.where(lane < 128 - shift, first, second)

    load_p_cols.wait()
    load_c_cols.wait()
    band_cols = from_lane(p_cols_v, row * 8 - 16)
    sub = lax.broadcasted_iota(I32, (32, 128), 0)
    place = jnp.full((32, 128), 4, I32)
    which = jnp.full((16, 128), 4, I32)
    pair = jnp.full((16, 128), 160, I32)
    for p in range(4):
        cols = band_cols[p : p + 1]
        column = cols - (row - 3) * 4
        place = jnp.where(column == sub, p, place)
        which = jnp.where(cols - (row - 1) * 4 == sub[:16], p, which)
        pair = jnp.where((column == 2 * sub[:16]) | (column == 2 * sub[:16] + 1), 4 * lane + p, pair)
    columns = jnp.clip(band_cols - (row - 3) * 4, 0, 27)
    target = from_lane(c_cols_v, row * 4 - 4) - (row - 3) * 4
    tab_v[PLACE : PLACE + 32] = place
    tab_v[PAIR : PAIR + 16] = pair
    tab_v[COLUMN : COLUMN + 4] = columns - (columns & 1)
    tab_v[WHICH : WHICH + 16] = which
    tab_v[TARGET : TARGET + 16] = jnp.where((target >= 0) & (target < 28), target, 28)

    left = lax.broadcasted_iota(I32, (128, 128), 1) < 64
    left16 = lax.broadcasted_iota(jnp.int16, (128, 128), 1) < 64

    def turn(x):
        return pltpu.roll(x.astype(F32), 64, 1).astype(x.dtype)

    load_p.wait()

    def halve(i, carry):
        for pair in range(2):
            x, y = p_own[i, 2 * pair], p_own[i, 2 * pair + 1]
            x_turned, y_turned = turn(x), turn(y)
            band[2, i, pair] = jnp.where(half == 0, jnp.where(left, x, y_turned), jnp.where(left, x_turned, y))
        return carry

    lax.fori_loop(0, 8, halve, 0)

    pl.semaphore_wait(barrier, 4 + jnp.where(above, 1 + core, 0) + jnp.where(below & jnp.logical_not(first), 2 - core, 0))

    @pl.when(last & (core == 1))
    def _():
        signal(gate, along_row(1))

    @pl.when(last)
    def _():
        signal(gate, along_row(2))


    def a_copy(i):
        return remote(a_hbm.at[i], a_far.at[i], a_send.at[i], a_recv.at[i], partner)

    cols_copy = remote(a_cols_hbm, far_cols_v, c_send, c_recv, partner)
    cols_copy.start()
    for i in range(8):
        a_copy(i).start()

    near = 3 - 2 * core

    def p_copy(kind, src, dst, n, device):
        return remote(band.at[src, n], band.at[dst, n], p_send.at[kind, n], p_recv.at[dst, n], device)

    def p_next(n):
        return p_copy(0, 2, 0, n, along_row(2))

    def p_prev(n):
        return p_copy(1, 2, 4, n, along_row(-2))

    def p_sibling(n):
        return p_copy(2, 2, 4 - near, n, sibling)

    def p_pass(n):
        return p_copy(3, 4 - 4 * core, near, n, sibling)

    for n in range(8):
        @pl.when(above)
        def _():
            p_next(n).start()

        @pl.when(below & jnp.logical_not(first))
        def _():
            p_prev(n).start()

    for n in range(8):
        p_sibling(n).start()

    to_smem = pltpu.make_async_copy(tab_v, tab, load_sem.at[5])
    to_smem.start()

    def transpose(i, carry):
        for q in range(4):
            p_turn[i, q] = p_own[i, q].T
        p_turn[i, 4] = jnp.zeros((128, 128), BF16)
        window[i, 28] = jnp.zeros((128, 128), BF16)
        return carry

    lax.fori_loop(0, 8, transpose, 0)
    spreadable[4] = jnp.zeros((128, 128), BF16)
    placed[160] = jnp.zeros((128, 128), BF16)
    to_smem.wait()

    def place_lines(slot, begin, count):
        def one(n, carry):
            line = slot * 8 + n
            for pair in range(2):
                x = band[slot, n, pair]
                turned = turn(x)
                spreadable[2 * pair] = jnp.where(left16, x, turned)
                spreadable[2 * pair + 1] = jnp.where(left16, turned, x)
            for p in range(4):
                column = tab[COLUMN + p, line]
                before = spreadable[tab[PLACE + column, line]]
                after = spreadable[tab[PLACE + 1 + column, line]]
                placed[4 * line + p] = jnp.where(left16, before, after)
            return carry

        lax.fori_loop(begin, begin + count, one, 0)

    def arrived(slot, n):
        p_copy(0, slot, slot, n, sibling).wait_recv()

    def there(slot):
        return jnp.where(slot > 2, above, below)

    def take(slot, n):
        @pl.when(there(slot))
        def _():
            arrived(slot, n)

            @pl.when(slot == 4 - 4 * core)
            def _():
                p_pass(n).start()

            place_lines(slot, n, 1)

    def follow(slot, n):
        @pl.when((n >= 0) & (slot == 4 - near) & there(slot))
        def _():
            arrived(slot, n)
            place_lines(slot, n, 1)

    place_lines(2, 0, 8)
    for n in range(8):
        arrived(near, n)
    place_lines(near, 0, 8)

    cols_copy.wait_recv()
    far_to_smem = pltpu.make_async_copy(far_cols_v, far_cols, load_sem.at[6])
    far_to_smem.start()
    load_own_cols.wait()
    load_a.wait()
    far_to_smem.wait()
    first_line = row * 8 - 16

    def fine_row(i, tiles):
        lhs = jnp.concatenate([a_own[i, s] for s in range(7)] + [a_far[i, s] for s in range(7)], axis=1)
        lines = [ref[s, 0, i] - first_line for ref in (own_cols, far_cols) for s in range(7)]
        lines = [jnp.clip(line, 0, 39) for line in lines]
        for n in tiles:
            rhs = jnp.concatenate(
                [
                    jnp.concatenate([placed[tab[PAIR + 2 * n + u, line]] for line in lines], axis=0)
                    for u in range(2)
                ],
                axis=1,
            )
            acc = jnp.dot(lhs, rhs, preferred_element_type=F32)
            for u in range(2):
                value = acc[:, u * 128 : (u + 1) * 128]
                high = value.astype(BF16).astype(F32)
                low = value - high
                window[i, 4 * n + 2 * u] = jnp.where(left, high, pltpu.roll(low, 64, 1)).astype(BF16)
                window[i, 4 * n + 2 * u + 1] = jnp.where(left, pltpu.roll(high, 64, 1), low).astype(BF16)

    def whole_row(i, carry):
        a_copy(i).wait_recv()
        fine_row(i, range(7))
        return carry

    def two_rows(i, carry):
        a_copy(2 * i).wait_recv()
        a_copy(2 * i + 1).wait_recv()
        fine_row(2 * i, range(7))
        fine_row(2 * i + 1, range(7))
        return carry

    @pl.when(jnp.logical_not(first))
    def _():
        def take_both(n, carry):
            take(4 - 4 * core, n)
            take(4 * core, n)
            follow(4 - near, n - 2)
            return carry

        lax.fori_loop(0, 8, take_both, 0)
        follow(4 - near, 6)
        follow(4 - near, 7)
        lax.fori_loop(0, 3, two_rows, 0)
        lax.fori_loop(6, 8, whole_row, 0)

    @pl.when(first)
    def _():
        def take_upper(n, carry):
            take(4, n)
            follow(3, n - 2)
            return carry

        def upper_row(i, carry):
            a_copy(i).wait_recv()
            fine_row(i, range(4, 7))
            take(0, i)
            follow(1, i - 2)
            return carry

        def lower_rows(i, carry):
            fine_row(2 * i, range(4))
            fine_row(2 * i + 1, range(4))
            return carry

        lax.fori_loop(0, 4, take_upper, 0)
        pl.semaphore_wait(gate, 2 - core)
        for n in range(8):
            p_prev(n).start()
        lax.fori_loop(4, 8, take_upper, 0)
        follow(3, 6)
        follow(3, 7)
        lax.fori_loop(0, 8, upper_row, 0)
        follow(1, 6)
        follow(1, 7)
        lax.fori_loop(0, 4, lower_rows, 0)

    def unit(n):
        early = n < 12
        return jnp.where(early, n // 3, n - 12), jnp.where(early, lax.rem(n, 3), 3)

    def steps(t):
        return jnp.where(t == 0, 2, jnp.where(t == 1, 1, jnp.where(t == 2, 3, 0)))

    def coarse_tiles(c, t):
        lhs = jnp.concatenate([p_turn[i, tab[WHICH + c, 16 + i]] for i in range(8)], axis=1)
        k = TARGET + lax.rem(grp + steps(t), 4) * 4
        tiles = []
        for pair in range(2):
            first = tab[k + 2 * pair, c]
            second = tab[k + 2 * pair + 1, c]
            rhs = jnp.concatenate(
                [jnp.concatenate([window[i, first], window[i, second]], axis=1) for i in range(8)], axis=0
            )
            acc = jnp.dot(lhs, rhs, preferred_element_type=F32)
            x, y = acc[:, :128], acc[:, 128:]
            tiles.append(jnp.where(left, x, y) + pltpu.roll(jnp.where(left, y, x), 64, 1))
        return tiles

    def outer_copy(n):
        return remote(outer.at[n], from_outer.at[n], s_send.at[0, n], s_recv.at[0, n], outside)

    def inner_copy(n):
        return remote(inner.at[n], from_inner.at[n], s_send.at[1, n], s_recv.at[1, n], sibling)

    def group_copy(c, t):
        return remote(
            center.at[3 * c + t], gathered.at[t, c], g_send.at[t, c], g_recv.at[t, c], along_grp(steps(t))
        )

    def fill(ref, n, c, t):
        for pair, tile in enumerate(coarse_tiles(c, t)):
            ref[n, pair] = tile

    def absorb(n):
        inner_copy(n).wait_recv()

        @pl.when(has_outer)
        def _():
            outer_copy(n).wait_recv()
            center[n] = center[n] + (from_outer[n] + from_inner[n])

        @pl.when(jnp.logical_not(has_outer))
        def _():
            center[n] = center[n] + from_inner[n]

    behind = jnp.where(first & (core == 0), BEHIND_FIRST, BEHIND)

    def one_unit(n, carry):
        c, t = unit(n)

        @pl.when(n >= behind)
        def _():
            absorb(n - behind)

        fill(outer, n, c + 8 * core, t)

        @pl.when(n >= behind)
        def _():
            done_c, done_t = unit(n - behind)
            group_copy(done_c, done_t).start()

        fill(inner, n, c + 8 - 8 * core, t)

        @pl.when(has_outer)
        def _():
            outer_copy(n).start()

        fill(center, n, c + 4, t)
        inner_copy(n).start()
        return carry

    lax.fori_loop(0, 16, one_unit, 0)

    def absorb_rest(n, carry):
        absorb(n)

        @pl.when((n > 16 - behind) & (n < 13))
        def _():
            done_c, done_t = unit(n - 1)
            group_copy(done_c, done_t).start()

        return carry

    lax.fori_loop(16 - behind, 16, absorb_rest, 0)

    for c in range(4):
        for t in range(3):
            group_copy(c, t).wait_recv()
        for pair in range(2):
            same = center[12 + c, pair] + gathered[0, c, pair]
            other = gathered[1, c, pair] + gathered[2, c, pair]
            x = jnp.where(half == 0, same, other)
            y = jnp.where(half == 0, other, same)
            out_v[c, 2 * pair] = jnp.where(left, x, pltpu.roll(y, 64, 1))
            out_v[c, 2 * pair + 1] = jnp.where(left, pltpu.roll(x, 64, 1), y)

    cols_copy.wait_send()
    for i in range(8):
        a_copy(i).wait_send()
    for n in range(8):
        p_sibling(n).wait_send()

        @pl.when(above)
        def _():
            p_next(n).wait_send()

        @pl.when(below)
        def _():
            p_prev(n).wait_send()

        @pl.when(there(4 - 4 * core))
        def _():
            p_pass(n).wait_send()

    def sent(n, carry):
        inner_copy(n).wait_send()

        @pl.when(has_outer)
        def _():
            outer_copy(n).wait_send()

        @pl.when(n < 12)
        def _():
            group_copy(n // 3, lax.rem(n, 3)).wait_send()

        return carry

    lax.fori_loop(0, 16, sent, 0)


def body(a_tiles, a_cols, p_tiles, p_cols, c_cols):
    operands = (a_cols.transpose(2, 1, 0), p_cols.T, c_cols.T, a_tiles.reshape(8, 7, 128, 128), p_tiles)
    dma = pltpu.SemaphoreType.DMA
    anywhere = pl.BlockSpec(memory_space=pl.ANY)
    side = pltpu.VMEM((16, 2, 128, 128), F32)
    return pl.pallas_call(
        kernel,
        out_shape=pltpu.VMEM((4, 4, 128, 128), F32),
        in_specs=[anywhere] * 5,
        out_specs=pl.BlockSpec(memory_space=pltpu.VMEM),
        scratch_shapes=[
            pltpu.VMEM((8, 7, 128, 128), BF16),
            pltpu.VMEM((8, 7, 128, 128), BF16),
            pltpu.VMEM((8, 4, 128, 128), BF16),
            pltpu.VMEM((8, 5, 128, 128), BF16),
            pltpu.VMEM((5, 8, 2, 128, 128), BF16),
            pltpu.VMEM((5, 128, 128), BF16),
            pltpu.VMEM((161, 128, 128), BF16),
            pltpu.VMEM((8, 29, 128, 128), BF16),
            side,
            side,
            side,
            side,
            side,
            pltpu.VMEM((3, 4, 2, 128, 128), F32),
            pltpu.VMEM((4, 1280), I32),
            pltpu.VMEM((16, 768), I32),
            pltpu.VMEM((7, 1, 8), I32),
            pltpu.VMEM((88, 128), I32),
            pltpu.SMEM((88, 128), I32),
            pltpu.SMEM((7, 1, 8), I32),
            pltpu.SMEM((7, 1, 8), I32),
            dma((7,)),
            dma((8,)),
            dma((8,)),
            dma,
            dma,
            dma((4, 8)),
            dma((5, 8)),
            dma((2, 16)),
            dma((2, 16)),
            dma((3, 4)),
            dma((3, 4)),
            pltpu.SemaphoreType.REGULAR,
        ],
        compiler_params=pltpu.CompilerParams(
            collective_id=0, has_side_effects=True, vmem_limit_bytes=52 * 1024 * 1024
        ),
        cost_estimate=pl.CostEstimate(flops=4_000_000_000, bytes_accessed=8_000_000, transcendentals=0),
    )(*[pltpu.with_memory_space_constraint(x, pltpu.HBM) for x in operands])


def solution(mesh):
    return jax.shard_map(
        body,
        mesh=mesh,
        in_specs=(
            P("row", "grp", None, None, None),
            P("row", "grp", None),
            P("row", None, None, None),
            P(),
            P(),
        ),
        out_specs=P("row", "grp", None, None),
        check_vma=False,
    )
```

```python
import jax
import jax.numpy as jnp
from jax import lax
from jax.experimental import pallas as pl
from jax.experimental.pallas import tpu as pltpu
from jax.sharding import PartitionSpec as P

MESH = pl.DeviceIdType.MESH
F32 = jnp.float32
BF16 = jnp.bfloat16
I32 = jnp.int32
PLACE, WHICH, TARGET, PAIR, COLUMN = 0, 32, 48, 64, 80
BEHIND = 4
BEHIND_FIRST = 8


def kernel(
    a_cols_hbm, p_cols_hbm, c_cols_hbm, a_hbm, p_hbm, out_v,
    a_own, a_far, p_own, p_turn, band, spreadable, placed, window, outer, inner,
    from_outer, from_inner, center, gathered, p_cols_v, c_cols_v, far_cols_v, tab_v, tab, own_cols, far_cols,
    load_sem, a_send, a_recv, c_send, c_recv, p_send, p_recv, s_send, s_recv, g_send, g_recv, gate,
):
    grp = lax.axis_index("grp")
    row = lax.axis_index("row")
    n_row = lax.axis_size("row")
    core = lax.rem(row, 2)
    half = lax.rem(grp, 2)

    def along_row(by):
        return (grp, lax.rem(row + by + n_row, n_row))

    def along_grp(by):
        return (lax.rem(grp + by, 4), row)

    partner = (jnp.where(core == 0, grp + 1 - 2 * half, 3 - grp), row)
    sibling = (grp, row + 1 - 2 * core)
    outside = along_row(2 * core - 1)

    def remote(src, dst, send, recv, device):
        return pltpu.make_async_remote_copy(
            src_ref=src, dst_ref=dst, send_sem=send, recv_sem=recv, device_id=device, device_id_type=MESH
        )

    load_p = pltpu.make_async_copy(p_hbm, p_own, load_sem.at[0])
    load_p_cols = pltpu.make_async_copy(p_cols_hbm, p_cols_v.at[:, pl.ds(128, 1024)], load_sem.at[1])
    load_c_cols = pltpu.make_async_copy(c_cols_hbm, c_cols_v.at[:, pl.ds(128, 512)], load_sem.at[2])
    load_a = pltpu.make_async_copy(a_hbm, a_own, load_sem.at[3])
    load_own_cols = pltpu.make_async_copy(a_cols_hbm, own_cols, load_sem.at[4])
    for load in (load_p, load_p_cols, load_c_cols, load_a, load_own_cols):
        load.start()

    place_z = lax.rem(row // 2, 16)
    below = row >= 2
    above = row < n_row - 2
    first = (place_z == 0) & below
    last = (place_z == 15) & above
    has_outer = jnp.where(core == 0, row, n_row - 1 - row) >= 2

    barrier = pltpu.get_barrier_semaphore()

    def signal(semaphore, peer):
        pl.semaphore_signal(semaphore, inc=1, device_id=peer, device_id_type=MESH)

    for by in (1, 2, 3):
        signal(barrier, along_grp(by))
    signal(barrier, sibling)

    @pl.when(below)
    def _():
        signal(barrier, along_row(-2))

    @pl.when(below & (core == 0))
    def _():
        signal(barrier, along_row(-1))

    @pl.when(above & jnp.logical_not(last))
    def _():
        signal(barrier, along_row(2))

    @pl.when(above & jnp.logical_not(last) & (core == 1))
    def _():
        signal(barrier, along_row(1))


    lane = lax.broadcasted_iota(I32, (1, 128), 1)

    def from_lane(ref, start):
        begin = start + 128
        tile = begin // 128
        shift = lax.rem(begin, 128)
        first = pltpu.roll(ref[:, pl.ds(pl.multiple_of(tile * 128, 128), 128)], 128 - shift, 1)
        second = pltpu.roll(ref[:, pl.ds(pl.multiple_of(tile * 128 + 128, 128), 128)], 128 - shift, 1)
        return jnp.where(lane < 128 - shift, first, second)

    load_p_cols.wait()
    load_c_cols.wait()
    band_cols = from_lane(p_cols_v, row * 8 - 16)
    sub = lax.broadcasted_iota(I32, (32, 128), 0)
    place = jnp.full((32, 128), 4, I32)
    which = jnp.full((16, 128), 4, I32)
    pair = jnp.full((16, 128), 160, I32)
    for p in range(4):
        cols = band_cols[p : p + 1]
        column = cols - (row - 3) * 4
        place = jnp.where(column == sub, p, place)
        which = jnp.where(cols - (row - 1) * 4 == sub[:16], p, which)
        pair = jnp.where((column == 2 * sub[:16]) | (column == 2 * sub[:16] + 1), 4 * lane + p, pair)
    columns = jnp.clip(band_cols - (row - 3) * 4, 0, 27)
    target = from_lane(c_cols_v, row * 4 - 4) - (row - 3) * 4
    tab_v[PLACE : PLACE + 32] = place
    tab_v[PAIR : PAIR + 16] = pair
    tab_v[COLUMN : COLUMN + 4] = columns - (columns & 1)
    tab_v[WHICH : WHICH + 16] = which
    tab_v[TARGET : TARGET + 16] = jnp.where((target >= 0) & (target < 28), target, 28)

    left = lax.broadcasted_iota(I32, (128, 128), 1) < 64
    left16 = lax.broadcasted_iota(jnp.int16, (128, 128), 1) < 64

    def turn(x):
        return pltpu.roll(x.astype(F32), 64, 1).astype(x.dtype)

    load_p.wait()

    def halve(i, carry):
        for pair in range(2):
            x, y = p_own[i, 2 * pair], p_own[i, 2 * pair + 1]
            x_turned, y_turned = turn(x), turn(y)
            band[2, i, pair] = jnp.where(half == 0, jnp.where(left, x, y_turned), jnp.where(left, x_turned, y))
        return carry

    lax.fori_loop(0, 8, halve, 0)

    pl.semaphore_wait(barrier, 4 + jnp.where(above, 1 + core, 0) + jnp.where(below & jnp.logical_not(first), 2 - core, 0))

    @pl.when(last & (core == 1))
    def _():
        signal(gate, along_row(1))

    @pl.when(last)
    def _():
        signal(gate, along_row(2))


    def a_copy(i):
        return remote(a_hbm.at[i], a_far.at[i], a_send.at[i], a_recv.at[i], partner)

    cols_copy = remote(a_cols_hbm, far_cols_v, c_send, c_recv, partner)
    cols_copy.start()
    for i in range(8):
        a_copy(i).start()

    near = 3 - 2 * core

    def p_copy(kind, src, dst, n, device):
        return remote(band.at[src, n], band.at[dst, n], p_send.at[kind, n], p_recv.at[dst, n], device)

    def p_next(n):
        return p_copy(0, 2, 0, n, along_row(2))

    def p_prev(n):
        return p_copy(1, 2, 4, n, along_row(-2))

    def p_sibling(n):
        return p_copy(2, 2, 4 - near, n, sibling)

    def p_pass(n):
        return p_copy(3, 4 - 4 * core, near, n, sibling)

    for n in range(8):
        @pl.when(above)
        def _():
            p_next(n).start()

        @pl.when(below & jnp.logical_not(first))
        def _():
            p_prev(n).start()

    for n in range(8):
        p_sibling(n).start()

    to_smem = pltpu.make_async_copy(tab_v, tab, load_sem.at[5])
    to_smem.start()

    def transpose(i, carry):
        for q in range(4):
            p_turn[i, q] = p_own[i, q].T
        p_turn[i, 4] = jnp.zeros((128, 128), BF16)
        window[i, 28] = jnp.zeros((128, 128), BF16)
        return carry

    lax.fori_loop(0, 8, transpose, 0)
    spreadable[4] = jnp.zeros((128, 128), BF16)
    placed[160] = jnp.zeros((128, 128), BF16)
    to_smem.wait()

    def place_lines(slot, begin, count):
        def one(n, carry):
            line = slot * 8 + n
            for pair in range(2):
                x = band[slot, n, pair]
                turned = turn(x)
                spreadable[2 * pair] = jnp.where(left16, x, turned)
                spreadable[2 * pair + 1] = jnp.where(left16, turned, x)
            for p in range(4):
                column = tab[COLUMN + p, line]
                before = spreadable[tab[PLACE + column, line]]
                after = spreadable[tab[PLACE + 1 + column, line]]
                placed[4 * line + p] = jnp.where(left16, before, after)
            return carry

        lax.fori_loop(begin, begin + count, one, 0)

    def arrived(slot, n):
        p_copy(0, slot, slot, n, sibling).wait_recv()

    def there(slot):
        return jnp.where(slot > 2, above, below)

    def take(slot, n):
        @pl.when(there(slot))
        def _():
            arrived(slot, n)

            @pl.when(slot == 4 - 4 * core)
            def _():
                p_pass(n).start()

            place_lines(slot, n, 1)

    def follow(slot, n):
        @pl.when((n >= 0) & (slot == 4 - near) & there(slot))
        def _():
            arrived(slot, n)
            place_lines(slot, n, 1)

    place_lines(2, 0, 8)
    for n in range(8):
        arrived(near, n)
    place_lines(near, 0, 8)

    cols_copy.wait_recv()
    far_to_smem = pltpu.make_async_copy(far_cols_v, far_cols, load_sem.at[6])
    far_to_smem.start()
    load_own_cols.wait()
    load_a.wait()
    far_to_smem.wait()
    first_line = row * 8 - 16

    def fine_row(i, tiles):
        lhs = jnp.concatenate([a_own[i, s] for s in range(7)] + [a_far[i, s] for s in range(7)], axis=1)
        lines = [ref[s, 0, i] - first_line for ref in (own_cols, far_cols) for s in range(7)]
        lines = [jnp.clip(line, 0, 39) for line in lines]
        for n in tiles:
            rhs = jnp.concatenate(
                [
                    jnp.concatenate([placed[tab[PAIR + 2 * n + u, line]] for line in lines], axis=0)
                    for u in range(2)
                ],
                axis=1,
            )
            acc = jnp.dot(lhs, rhs, preferred_element_type=F32)
            for u in range(2):
                value = acc[:, u * 128 : (u + 1) * 128]
                high = value.astype(BF16).astype(F32)
                low = value - high
                window[i, 4 * n + 2 * u] = jnp.where(left, high, pltpu.roll(low, 64, 1)).astype(BF16)
                window[i, 4 * n + 2 * u + 1] = jnp.where(left, pltpu.roll(high, 64, 1), low).astype(BF16)

    def whole_row(i, carry):
        a_copy(i).wait_recv()
        fine_row(i, range(7))
        return carry

    def two_rows(i, carry):
        a_copy(2 * i).wait_recv()
        a_copy(2 * i + 1).wait_recv()
        fine_row(2 * i, range(7))
        fine_row(2 * i + 1, range(7))
        return carry

    def tiles_of_two(tiles):
        def two(i, carry):
            fine_row(2 * i, tiles)
            fine_row(2 * i + 1, tiles)
            return carry

        return two

    @pl.when(jnp.logical_not(first | last))
    def _():
        def take_both(n, carry):
            take(4 - 4 * core, n)
            take(4 * core, n)
            follow(4 - near, n - 2)
            return carry

        lax.fori_loop(0, 8, take_both, 0)
        follow(4 - near, 6)
        follow(4 - near, 7)
        lax.fori_loop(0, 3, two_rows, 0)
        lax.fori_loop(6, 8, whole_row, 0)

    @pl.when(last)
    def _():
        def take_late(n, carry):
            take(0, n)
            follow(1, n - 2)

            @pl.when(n >= 2)
            def _():
                take(4, n - 2)

            follow(3, n - 4)
            return carry

        lax.fori_loop(0, 8, take_late, 0)
        follow(1, 6)
        follow(1, 7)
        for i in range(4):
            a_copy(i).wait_recv()

        def early(i, carry):
            take(4, 6 + i)
            return tiles_of_two(range(3))(i, carry)

        lax.fori_loop(0, 2, early, 0)
        for n in range(4, 8):
            follow(3, n)
        lax.fori_loop(0, 2, tiles_of_two(range(3, 7)), 0)
        lax.fori_loop(2, 3, two_rows, 0)
        lax.fori_loop(6, 8, whole_row, 0)

    @pl.when(first)
    def _():
        def take_upper(n, carry):
            take(4, n)
            follow(3, n - 2)
            return carry

        def upper_row(i, carry):
            a_copy(i).wait_recv()
            fine_row(i, range(4, 7))
            take(0, i)
            follow(1, i - 2)
            return carry

        lax.fori_loop(0, 4, take_upper, 0)
        pl.semaphore_wait(gate, 2 - core)
        for n in range(8):
            p_prev(n).start()
        lax.fori_loop(4, 8, take_upper, 0)
        follow(3, 6)
        follow(3, 7)
        lax.fori_loop(0, 8, upper_row, 0)
        follow(1, 6)
        follow(1, 7)
        lax.fori_loop(0, 4, tiles_of_two(range(4)), 0)

    def unit(n):
        early = n < 12
        return jnp.where(early, n // 3, n - 12), jnp.where(early, lax.rem(n, 3), 3)

    def steps(t):
        return jnp.where(t == 0, 2, jnp.where(t == 1, 1, jnp.where(t == 2, 3, 0)))

    def coarse_tiles(c, t):
        lhs = jnp.concatenate([p_turn[i, tab[WHICH + c, 16 + i]] for i in range(8)], axis=1)
        k = TARGET + lax.rem(grp + steps(t), 4) * 4
        tiles = []
        for pair in range(2):
            first = tab[k + 2 * pair, c]
            second = tab[k + 2 * pair + 1, c]
            rhs = jnp.concatenate(
                [jnp.concatenate([window[i, first], window[i, second]], axis=1) for i in range(8)], axis=0
            )
            acc = jnp.dot(lhs, rhs, preferred_element_type=F32)
            x, y = acc[:, :128], acc[:, 128:]
            tiles.append(jnp.where(left, x, y) + pltpu.roll(jnp.where(left, y, x), 64, 1))
        return tiles

    def outer_copy(n):
        return remote(outer.at[n], from_outer.at[n], s_send.at[0, n], s_recv.at[0, n], outside)

    def inner_copy(n):
        return remote(inner.at[n], from_inner.at[n], s_send.at[1, n], s_recv.at[1, n], sibling)

    def group_copy(c, t):
        return remote(
            center.at[3 * c + t], gathered.at[t, c], g_send.at[t, c], g_recv.at[t, c], along_grp(steps(t))
        )

    def fill(ref, n, c, t):
        for pair, tile in enumerate(coarse_tiles(c, t)):
            ref[n, pair] = tile

    def absorb(n):
        inner_copy(n).wait_recv()

        @pl.when(has_outer)
        def _():
            outer_copy(n).wait_recv()
            center[n] = center[n] + (from_outer[n] + from_inner[n])

        @pl.when(jnp.logical_not(has_outer))
        def _():
            center[n] = center[n] + from_inner[n]

    behind = jnp.where(first & (core == 0), BEHIND_FIRST, BEHIND)

    def one_unit(n, carry):
        c, t = unit(n)

        @pl.when(n >= behind)
        def _():
            absorb(n - behind)

        fill(outer, n, c + 8 * core, t)

        @pl.when(n >= behind)
        def _():
            done_c, done_t = unit(n - behind)
            group_copy(done_c, done_t).start()

        @pl.when(has_outer)
        def _():
            outer_copy(n).start()

        fill(inner, n, c + 8 - 8 * core, t)
        fill(center, n, c + 4, t)
        inner_copy(n).start()
        return carry

    lax.fori_loop(0, 16, one_unit, 0)

    def absorb_rest(n, carry):
        absorb(n)

        @pl.when((n > 16 - behind) & (n < 13))
        def _():
            done_c, done_t = unit(n - 1)
            group_copy(done_c, done_t).start()

        return carry

    lax.fori_loop(16 - behind, 16, absorb_rest, 0)

    for c in range(4):
        for t in range(3):
            group_copy(c, t).wait_recv()
        for pair in range(2):
            same = center[12 + c, pair] + gathered[0, c, pair]
            other = gathered[1, c, pair] + gathered[2, c, pair]
            x = jnp.where(half == 0, same, other)
            y = jnp.where(half == 0, other, same)
            out_v[c, 2 * pair] = jnp.where(left, x, pltpu.roll(y, 64, 1))
            out_v[c, 2 * pair + 1] = jnp.where(left, pltpu.roll(x, 64, 1), y)

    cols_copy.wait_send()
    for i in range(8):
        a_copy(i).wait_send()
    for n in range(8):
        p_sibling(n).wait_send()

        @pl.when(above)
        def _():
            p_next(n).wait_send()

        @pl.when(below)
        def _():
            p_prev(n).wait_send()

        @pl.when(there(4 - 4 * core))
        def _():
            p_pass(n).wait_send()

    def sent(n, carry):
        inner_copy(n).wait_send()

        @pl.when(has_outer)
        def _():
            outer_copy(n).wait_send()

        @pl.when(n < 12)
        def _():
            group_copy(n // 3, lax.rem(n, 3)).wait_send()

        return carry

    lax.fori_loop(0, 16, sent, 0)


def body(a_tiles, a_cols, p_tiles, p_cols, c_cols):
    operands = (a_cols.transpose(2, 1, 0), p_cols.T, c_cols.T, a_tiles.reshape(8, 7, 128, 128), p_tiles)
    dma = pltpu.SemaphoreType.DMA
    anywhere = pl.BlockSpec(memory_space=pl.ANY)
    side = pltpu.VMEM((16, 2, 128, 128), F32)
    return pl.pallas_call(
        kernel,
        out_shape=pltpu.VMEM((4, 4, 128, 128), F32),
        in_specs=[anywhere] * 5,
        out_specs=pl.BlockSpec(memory_space=pltpu.VMEM),
        scratch_shapes=[
            pltpu.VMEM((8, 7, 128, 128), BF16),
            pltpu.VMEM((8, 7, 128, 128), BF16),
            pltpu.VMEM((8, 4, 128, 128), BF16),
            pltpu.VMEM((8, 5, 128, 128), BF16),
            pltpu.VMEM((5, 8, 2, 128, 128), BF16),
            pltpu.VMEM((5, 128, 128), BF16),
            pltpu.VMEM((161, 128, 128), BF16),
            pltpu.VMEM((8, 29, 128, 128), BF16),
            side,
            side,
            side,
            side,
            side,
            pltpu.VMEM((3, 4, 2, 128, 128), F32),
            pltpu.VMEM((4, 1280), I32),
            pltpu.VMEM((16, 768), I32),
            pltpu.VMEM((7, 1, 8), I32),
            pltpu.VMEM((88, 128), I32),
            pltpu.SMEM((88, 128), I32),
            pltpu.SMEM((7, 1, 8), I32),
            pltpu.SMEM((7, 1, 8), I32),
            dma((7,)),
            dma((8,)),
            dma((8,)),
            dma,
            dma,
            dma((4, 8)),
            dma((5, 8)),
            dma((2, 16)),
            dma((2, 16)),
            dma((3, 4)),
            dma((3, 4)),
            pltpu.SemaphoreType.REGULAR,
        ],
        compiler_params=pltpu.CompilerParams(
            collective_id=0, has_side_effects=True, vmem_limit_bytes=52 * 1024 * 1024
        ),
        cost_estimate=pl.CostEstimate(flops=4_000_000_000, bytes_accessed=8_000_000, transcendentals=0),
    )(*[pltpu.with_memory_space_constraint(x, pltpu.HBM) for x in operands])


def solution(mesh):
    return jax.shard_map(
        body,
        mesh=mesh,
        in_specs=(
            P("row", "grp", None, None, None),
            P("row", "grp", None),
            P("row", None, None, None),
            P(),
            P(),
        ),
        out_specs=P("row", "grp", None, None),
        check_vma=False,
    )
```

```python
import jax
import jax.numpy as jnp
from jax import lax
from jax.experimental import pallas as pl
from jax.experimental.pallas import tpu as pltpu
from jax.sharding import PartitionSpec as P

MESH = pl.DeviceIdType.MESH
F32 = jnp.float32
BF16 = jnp.bfloat16
I32 = jnp.int32
PLACE, WHICH, TARGET, PAIR, COLUMN = 0, 32, 48, 64, 80
BEHIND = 4
BEHIND_FIRST = 8


def kernel(
    a_cols_hbm, p_cols_hbm, c_cols_hbm, a_hbm, p_hbm, out_v,
    a_own, a_far, p_own, p_turn, band, begun, spreadable, placed, window, outer, inner,
    from_outer, from_inner, center, gathered, terms, terms_in, sums, sums_in, p_cols_v, c_cols_v, far_cols_v, tab_v, tab, own_cols, far_cols,
    load_sem, a_send, a_recv, c_send, c_recv, p_send, p_recv, s_send, s_recv, g_send, g_recv, t_send, t_recv, gate,
):
    grp = lax.axis_index("grp")
    row = lax.axis_index("row")
    n_row = lax.axis_size("row")
    core = lax.rem(row, 2)
    half = lax.rem(grp, 2)

    def along_row(by):
        return (grp, lax.rem(row + by + n_row, n_row))

    def along_grp(by):
        return (lax.rem(grp + by, 4), row)

    partner = (jnp.where(core == 0, grp + 1 - 2 * half, 3 - grp), row)
    sibling = (grp, row + 1 - 2 * core)
    outside = along_row(2 * core - 1)

    def remote(src, dst, send, recv, device):
        return pltpu.make_async_remote_copy(
            src_ref=src, dst_ref=dst, send_sem=send, recv_sem=recv, device_id=device, device_id_type=MESH
        )

    load_p = pltpu.make_async_copy(p_hbm, p_own, load_sem.at[0])
    load_p_cols = pltpu.make_async_copy(p_cols_hbm, p_cols_v.at[:, pl.ds(128, 1024)], load_sem.at[1])
    load_c_cols = pltpu.make_async_copy(c_cols_hbm, c_cols_v.at[:, pl.ds(128, 512)], load_sem.at[2])
    load_a = pltpu.make_async_copy(a_hbm, a_own, load_sem.at[3])
    load_own_cols = pltpu.make_async_copy(a_cols_hbm, own_cols, load_sem.at[4])
    for load in (load_p, load_p_cols, load_c_cols, load_a, load_own_cols):
        load.start()

    place_z = lax.rem(row // 2, 16)
    below = row >= 2
    above = row < n_row - 2
    first = (place_z == 0) & below
    last = (place_z == 15) & above
    has_outer = jnp.where(core == 0, row, n_row - 1 - row) >= 2

    barrier = pltpu.get_barrier_semaphore()

    def signal(semaphore, peer):
        pl.semaphore_signal(semaphore, inc=1, device_id=peer, device_id_type=MESH)

    for by in (1, 2, 3):
        signal(barrier, along_grp(by))
    signal(barrier, sibling)

    @pl.when(below)
    def _():
        signal(barrier, along_row(-2))

    @pl.when(below & (core == 0))
    def _():
        signal(barrier, along_row(-1))

    @pl.when(above & jnp.logical_not(last))
    def _():
        signal(barrier, along_row(2))

    @pl.when(above & jnp.logical_not(last) & (core == 1))
    def _():
        signal(barrier, along_row(1))


    lane = lax.broadcasted_iota(I32, (1, 128), 1)

    def from_lane(ref, start):
        begin = start + 128
        tile = begin // 128
        shift = lax.rem(begin, 128)
        first = pltpu.roll(ref[:, pl.ds(pl.multiple_of(tile * 128, 128), 128)], 128 - shift, 1)
        second = pltpu.roll(ref[:, pl.ds(pl.multiple_of(tile * 128 + 128, 128), 128)], 128 - shift, 1)
        return jnp.where(lane < 128 - shift, first, second)

    load_p_cols.wait()
    load_c_cols.wait()
    band_cols = from_lane(p_cols_v, row * 8 - 16)
    sub = lax.broadcasted_iota(I32, (32, 128), 0)
    place = jnp.full((32, 128), 4, I32)
    which = jnp.full((16, 128), 4, I32)
    pair = jnp.full((16, 128), 160, I32)
    for p in range(4):
        cols = band_cols[p : p + 1]
        column = cols - (row - 3) * 4
        place = jnp.where(column == sub, p, place)
        which = jnp.where(cols - (row - 1) * 4 == sub[:16], p, which)
        pair = jnp.where((column == 2 * sub[:16]) | (column == 2 * sub[:16] + 1), 4 * lane + p, pair)
    columns = jnp.clip(band_cols - (row - 3) * 4, 0, 27)
    target = from_lane(c_cols_v, row * 4 - 4) - (row - 3) * 4
    tab_v[PLACE : PLACE + 32] = place
    tab_v[PAIR : PAIR + 16] = pair
    tab_v[COLUMN : COLUMN + 4] = columns - (columns & 1)
    tab_v[WHICH : WHICH + 16] = which
    tab_v[TARGET : TARGET + 16] = jnp.where((target >= 0) & (target < 28), target, 28)

    left = lax.broadcasted_iota(I32, (128, 128), 1) < 64
    left16 = lax.broadcasted_iota(jnp.int16, (128, 128), 1) < 64

    def turn(x):
        return pltpu.roll(x.astype(F32), 64, 1).astype(x.dtype)

    load_p.wait()

    def halve(i, carry):
        for pair in range(2):
            x, y = p_own[i, 2 * pair], p_own[i, 2 * pair + 1]
            x_turned, y_turned = turn(x), turn(y)
            band[2, i, pair] = jnp.where(half == 0, jnp.where(left, x, y_turned), jnp.where(left, x_turned, y))
        return carry

    lax.fori_loop(0, 8, halve, 0)

    pl.semaphore_wait(barrier, 4 + jnp.where(above, 1 + core, 0) + jnp.where(below & jnp.logical_not(first), 2 - core, 0))

    @pl.when(last & (core == 1))
    def _():
        signal(gate, along_row(1))

    @pl.when(last)
    def _():
        signal(gate, along_row(2))


    def a_copy(i):
        return remote(a_hbm.at[i], a_far.at[i], a_send.at[i], a_recv.at[i], partner)

    def last_copy(part):
        slots = pl.ds(5 * part, 5 - 3 * part)
        return remote(a_hbm.at[7, slots], a_far.at[7, slots], a_send.at[7 + part], a_recv.at[7 + part], partner)

    cols_copy = remote(a_cols_hbm, far_cols_v, c_send, c_recv, partner)
    cols_copy.start()
    for i in range(7):
        a_copy(i).start()
    for part in range(2):
        last_copy(part).start()

    near = 3 - 2 * core

    def p_copy(kind, src, dst, n, device):
        return remote(band.at[src, n], band.at[dst, n], p_send.at[kind, n], p_recv.at[dst, n], device)

    def p_next(n):
        return p_copy(0, 2, 0, n, along_row(2))

    def p_prev(n):
        return p_copy(1, 2, 4, n, along_row(-2))

    def p_sibling(n):
        return p_copy(2, 2, 4 - near, n, sibling)

    def p_pass(n):
        return p_copy(3, 4 - 4 * core, near, n, sibling)

    def start_all(copy):
        def one(n, carry):
            copy(n).start()
            return carry

        lax.fori_loop(0, 8, one, 0)

    @pl.when(above & (core == 1))
    def _():
        start_all(p_next)

    @pl.when(below & jnp.logical_not(first) & (core == 0))
    def _():
        start_all(p_prev)

    start_all(p_sibling)

    to_smem = pltpu.make_async_copy(tab_v, tab, load_sem.at[5])
    to_smem.start()

    def transpose(i, carry):
        for q in range(4):
            p_turn[i, q] = p_own[i, q].T
        p_turn[i, 4] = jnp.zeros((128, 128), BF16)
        window[i, 28] = jnp.zeros((128, 128), BF16)
        return carry

    lax.fori_loop(0, 8, transpose, 0)
    spreadable[4] = jnp.zeros((128, 128), BF16)
    placed[160] = jnp.zeros((128, 128), BF16)
    to_smem.wait()

    def place_lines(slot, begin, count):
        def one(n, carry):
            line = slot * 8 + n
            for pair in range(2):
                x = band[slot, n, pair]
                turned = turn(x)
                spreadable[2 * pair] = jnp.where(left16, x, turned)
                spreadable[2 * pair + 1] = jnp.where(left16, turned, x)
            for p in range(4):
                column = tab[COLUMN + p, line]
                before = spreadable[tab[PLACE + column, line]]
                after = spreadable[tab[PLACE + 1 + column, line]]
                placed[4 * line + p] = jnp.where(left16, before, after)
            return carry

        lax.fori_loop(begin, begin + count, one, 0)

    def arrived(slot, n):
        p_copy(0, slot, slot, n, sibling).wait_recv()

    def there(slot):
        return jnp.where(slot > 2, above, below)

    def take(slot, n):
        @pl.when(there(slot))
        def _():
            arrived(slot, n)

            @pl.when(slot == 4 - 4 * core)
            def _():
                p_pass(n).start()

            place_lines(slot, n, 1)

    def follow(slot, n):
        @pl.when((n >= 0) & (slot == 4 - near) & there(slot))
        def _():
            arrived(slot, n)
            place_lines(slot, n, 1)

    place_lines(2, 0, 8)
    for n in range(8):
        arrived(near, n)
    place_lines(near, 0, 8)

    cols_copy.wait_recv()
    far_to_smem = pltpu.make_async_copy(far_cols_v, far_cols, load_sem.at[6])
    far_to_smem.start()
    load_own_cols.wait()
    load_a.wait()
    far_to_smem.wait()
    first_line = row * 8 - 16

    def tile_maker(i, slots):
        lhs = jnp.concatenate([(a_own if s < 7 else a_far)[i, s % 7] for s in slots], axis=1)
        lines = [(own_cols if s < 7 else far_cols)[s % 7, 0, i] - first_line for s in slots]
        lines = [jnp.clip(line, 0, 39) for line in lines]

        def tile(n):
            rhs = jnp.concatenate(
                [
                    jnp.concatenate([placed[tab[PAIR + 2 * n + u, line]] for line in lines], axis=0)
                    for u in range(2)
                ],
                axis=1,
            )
            return jnp.dot(lhs, rhs, preferred_element_type=F32)

        return tile

    def split(i, n, acc):
        for u in range(2):
            value = acc[:, u * 128 : (u + 1) * 128]
            high = value.astype(BF16).astype(F32)
            low = value - high
            window[i, 4 * n + 2 * u] = jnp.where(left, high, pltpu.roll(low, 64, 1)).astype(BF16)
            window[i, 4 * n + 2 * u + 1] = jnp.where(left, pltpu.roll(high, 64, 1), low).astype(BF16)

    def fine_row(i, begin, count):
        tile = tile_maker(i, range(14))
        for n in [begin + k for k in range(count)]:
            split(i, n, tile(n))

    def last_row():
        last_copy(0).wait_recv()
        tile = tile_maker(7, range(12))
        for n in range(7):
            begun[n] = tile(n)
        last_copy(1).wait_recv()
        tile = tile_maker(7, range(12, 14))
        for n in range(7):
            split(7, n, begun[n] + tile(n))

    ahead = first & (core == 0)
    late_near = last & (core == 0)
    late_follow = last & (core == 1)

    def follow_all(n, carry):
        follow(4 - near, n)

        @pl.when((n == 3) & late_near)
        def _():
            start_all(p_next)

        return carry

    def take_near(n, carry):
        take(4 - 4 * core, n)

        @pl.when(jnp.logical_not(ahead | last))
        def _():
            follow(4 - near, n - 2)

        @pl.when((n == 5) & above & (core == 0) & jnp.logical_not(last))
        def _():
            start_all(p_next)

        @pl.when((n == 5) & below & (core == 1))
        def _():
            @pl.when(first)
            def _():
                pl.semaphore_wait(gate, 1)

            start_all(p_prev)

        return carry

    def take_far(n, carry):
        take(4 * core, n)
        return carry

    def four_tiles(i, carry):
        a_copy(2 * i).wait_recv()
        a_copy(2 * i + 1).wait_recv()
        fine_row(2 * i, 3 - 3 * core, 4)
        fine_row(2 * i + 1, 3 - 3 * core, 4)
        return carry

    def other_three_tiles(i, carry):
        fine_row(2 * i, 4 * core, 3)
        fine_row(2 * i + 1, 4 * core, 3)
        return carry

    def three_tiles(i, carry):
        a_copy(2 * i).wait_recv()
        a_copy(2 * i + 1).wait_recv()
        fine_row(2 * i, 0, 3)
        fine_row(2 * i + 1, 0, 3)
        return carry

    def other_four_tiles(i, carry):
        fine_row(2 * i, 3, 4)
        fine_row(2 * i + 1, 3, 4)
        return carry

    def two_rows(i, carry):
        a_copy(2 * i).wait_recv()
        a_copy(2 * i + 1).wait_recv()
        fine_row(2 * i, 0, 7)
        fine_row(2 * i + 1, 0, 7)
        return carry

    def whole_row(i, carry):
        a_copy(i).wait_recv()
        fine_row(i, 0, 7)
        return carry

    @pl.when(late_near)
    def _():
        lax.fori_loop(0, 8, follow_all, 0)

    lax.fori_loop(0, 8, take_near, 0)

    @pl.when(ahead)
    def _():
        pl.semaphore_wait(gate, 2)
        start_all(p_prev)
        lax.fori_loop(0, 8, follow_all, 0)

    @pl.when(jnp.logical_not(ahead | last))
    def _():
        follow(4 - near, 6)
        follow(4 - near, 7)

    pairs = jnp.where(ahead, 3, 2)

    @pl.when(late_follow)
    def _():
        lax.fori_loop(0, 2, three_tiles, 0)
        lax.fori_loop(0, 8, follow_all, 0)
        lax.fori_loop(0, 8, take_far, 0)
        lax.fori_loop(0, 2, other_four_tiles, 0)

    @pl.when(jnp.logical_not(late_follow))
    def _():
        lax.fori_loop(0, pairs, four_tiles, 0)
        lax.fori_loop(0, 8, take_far, 0)
        lax.fori_loop(0, pairs, other_three_tiles, 0)

    lax.fori_loop(pairs, 3, two_rows, 0)

    whole_row(6, 0)

    @pl.when(jnp.logical_not(last))
    def _():
        last_row()

    @pl.when(last)
    def _():
        last_copy(0).wait_recv()
        last_copy(1).wait_recv()
        fine_row(7, 0, 7)

    def unit(n):
        early = n < 12
        return jnp.where(early, n // 3, n - 12), jnp.where(early, lax.rem(n, 3), 3)

    def steps(t):
        return jnp.where(t == 0, 2, jnp.where(t == 1, 1, jnp.where(t == 2, 3, 0)))

    def coarse_tiles(c, t):
        lhs = jnp.concatenate([p_turn[i, tab[WHICH + c, 16 + i]] for i in range(8)], axis=1)
        k = TARGET + lax.rem(grp + steps(t), 4) * 4
        tiles = []
        for pair in range(2):
            first = tab[k + 2 * pair, c]
            second = tab[k + 2 * pair + 1, c]
            rhs = jnp.concatenate(
                [jnp.concatenate([window[i, first], window[i, second]], axis=1) for i in range(8)], axis=0
            )
            acc = jnp.dot(lhs, rhs, preferred_element_type=F32)
            x, y = acc[:, :128], acc[:, 128:]
            tiles.append(jnp.where(left, x, y) + pltpu.roll(jnp.where(left, y, x), 64, 1))
        return tiles

    def outer_copy(n):
        return remote(outer.at[n], from_outer.at[n], s_send.at[0, n], s_recv.at[0, n], outside)

    sums_first = last & (core == 1)
    gets_sums = first & (core == 0)

    def by_sums(n):
        return unit(n)[0] == 3

    def sends_outer(n):
        return has_outer & jnp.logical_not(sums_first & by_sums(n))

    def gets_outer(n):
        return has_outer & jnp.logical_not(gets_sums & by_sums(n))

    def term_copy(t):
        return remote(terms.at[t], terms_in.at[t], t_send.at[t], t_recv.at[t], along_grp(steps(t)))

    def sums_copy():
        return remote(sums, sums_in, t_send.at[3], t_recv.at[3], outside)

    def whole_tiles(own, from_two, from_one, from_three):
        same = own + from_two
        other = from_one + from_three
        x = jnp.where(half == 0, same, other)
        y = jnp.where(half == 0, other, same)
        return jnp.where(left, x, pltpu.roll(y, 64, 1)), jnp.where(left, pltpu.roll(x, 64, 1), y)

    def inner_copy(n):
        return remote(inner.at[n], from_inner.at[n], s_send.at[1, n], s_recv.at[1, n], sibling)

    def group_copy(c, t):
        return remote(
            center.at[3 * c + t], gathered.at[t, c], g_send.at[t, c], g_recv.at[t, c], along_grp(steps(t))
        )

    def fill(ref, n, c, t):
        for pair, tile in enumerate(coarse_tiles(c, t)):
            ref[n, pair] = tile

    def absorb(n):
        inner_copy(n).wait_recv()

        @pl.when(gets_outer(n))
        def _():
            outer_copy(n).wait_recv()

        center[n] = center[n] + (from_inner[n] + jnp.where(gets_outer(n), from_outer[n], 0.0))

    behind = jnp.where(first & (core == 0), BEHIND_FIRST, BEHIND)

    def sum_first(n):
        @pl.when(n < 4)
        def _():
            fill(terms, n, 11, n)

        @pl.when((n > 0) & (n < 4))
        def _():
            term_copy(n - 1).start()

        @pl.when(n == 8)
        def _():
            for t in range(3):
                term_copy(t).wait_recv()
            for pair in range(2):
                tiles = whole_tiles(terms[3, pair], terms_in[0, pair], terms_in[1, pair], terms_in[2, pair])
                sums[2 * pair], sums[2 * pair + 1] = tiles

        @pl.when(n == 9)
        def _():
            sums_copy().start()

    def one_unit(n, carry):
        c, t = unit(n)

        @pl.when(n >= behind)
        def _():
            absorb(n - behind)

        fill(outer, n, c + 8 * core, t)

        @pl.when(n >= behind)
        def _():
            done_c, done_t = unit(n - behind)
            group_copy(done_c, done_t).start()

        @pl.when(sends_outer(n))
        def _():
            outer_copy(n).start()

        fill(inner, n, c + 8 - 8 * core, t)
        fill(center, n, c + 4, t)
        inner_copy(n).start()

        @pl.when(sums_first)
        def _():
            sum_first(n)

        return carry

    lax.fori_loop(0, 16, one_unit, 0)

    cols_copy.wait_send()
    for i in range(7):
        a_copy(i).wait_send()
    for part in range(2):
        last_copy(part).wait_send()
    for n in range(8):
        p_sibling(n).wait_send()

        @pl.when(above)
        def _():
            p_next(n).wait_send()

        @pl.when(below)
        def _():
            p_prev(n).wait_send()

        @pl.when(there(4 - 4 * core))
        def _():
            p_pass(n).wait_send()

    def finish(c):
        for t in range(3):
            group_copy(c, t).wait_recv()
        for pair in range(2):
            tiles = whole_tiles(
                center[12 + c, pair], gathered[0, c, pair], gathered[1, c, pair], gathered[2, c, pair]
            )
            out_v[c, 2 * pair], out_v[c, 2 * pair + 1] = tiles

    def absorb_rest(n, carry):
        absorb(n)

        @pl.when((n > 16 - behind) & (n < 13))
        def _():
            done_c, done_t = unit(n - 1)
            group_copy(done_c, done_t).start()

        @pl.when(n >= 13)
        def _():
            finish(n - 13)

        return carry

    lax.fori_loop(16 - behind, 15, absorb_rest, 0)
    finish(2)

    def sent(n, carry):
        inner_copy(n).wait_send()

        @pl.when(sends_outer(n))
        def _():
            outer_copy(n).wait_send()

        @pl.when(n < 9)
        def _():
            group_copy(n // 3, lax.rem(n, 3)).wait_send()

        return carry

    lax.fori_loop(0, 15, sent, 0)
    absorb(15)
    finish(3)

    @pl.when(gets_sums)
    def _():
        sums_copy().wait_recv()
        out_v[3] = out_v[3] + sums_in[...]

    @pl.when(sums_first)
    def _():
        for t in range(3):
            term_copy(t).wait_send()
        sums_copy().wait_send()

    sent(15, 0)
    for t in range(3):
        group_copy(3, t).wait_send()


def body(a_tiles, a_cols, p_tiles, p_cols, c_cols):
    operands = (a_cols.transpose(2, 1, 0), p_cols.T, c_cols.T, a_tiles.reshape(8, 7, 128, 128), p_tiles)
    dma = pltpu.SemaphoreType.DMA
    anywhere = pl.BlockSpec(memory_space=pl.ANY)
    side = pltpu.VMEM((16, 2, 128, 128), F32)
    return pl.pallas_call(
        kernel,
        out_shape=pltpu.VMEM((4, 4, 128, 128), F32),
        in_specs=[anywhere] * 5,
        out_specs=pl.BlockSpec(memory_space=pltpu.VMEM),
        scratch_shapes=[
            pltpu.VMEM((8, 7, 128, 128), BF16),
            pltpu.VMEM((8, 7, 128, 128), BF16),
            pltpu.VMEM((8, 4, 128, 128), BF16),
            pltpu.VMEM((8, 5, 128, 128), BF16),
            pltpu.VMEM((5, 8, 2, 128, 128), BF16),
            pltpu.VMEM((7, 128, 256), F32),
            pltpu.VMEM((5, 128, 128), BF16),
            pltpu.VMEM((161, 128, 128), BF16),
            pltpu.VMEM((8, 29, 128, 128), BF16),
            side,
            side,
            side,
            side,
            side,
            pltpu.VMEM((3, 4, 2, 128, 128), F32),
            pltpu.VMEM((4, 2, 128, 128), F32),
            pltpu.VMEM((3, 2, 128, 128), F32),
            pltpu.VMEM((4, 128, 128), F32),
            pltpu.VMEM((4, 128, 128), F32),
            pltpu.VMEM((4, 1280), I32),
            pltpu.VMEM((16, 768), I32),
            pltpu.VMEM((7, 1, 8), I32),
            pltpu.VMEM((88, 128), I32),
            pltpu.SMEM((88, 128), I32),
            pltpu.SMEM((7, 1, 8), I32),
            pltpu.SMEM((7, 1, 8), I32),
            dma((7,)),
            dma((9,)),
            dma((9,)),
            dma,
            dma,
            dma((4, 8)),
            dma((5, 8)),
            dma((2, 16)),
            dma((2, 16)),
            dma((3, 4)),
            dma((3, 4)),
            dma((4,)),
            dma((4,)),
            pltpu.SemaphoreType.REGULAR,
        ],
        compiler_params=pltpu.CompilerParams(
            collective_id=0, has_side_effects=True, vmem_limit_bytes=52 * 1024 * 1024
        ),
        cost_estimate=pl.CostEstimate(flops=4_000_000_000, bytes_accessed=8_000_000, transcendentals=0),
    )(*[pltpu.with_memory_space_constraint(x, pltpu.HBM) for x in operands])


def solution(mesh):
    return jax.shard_map(
        body,
        mesh=mesh,
        in_specs=(
            P("row", "grp", None, None, None),
            P("row", "grp", None),
            P("row", None, None, None),
            P(),
            P(),
        ),
        out_specs=P("row", "grp", None, None),
        check_vma=False,
    )
```

```python
import jax
import jax.numpy as jnp
from jax import lax
from jax.experimental import pallas as pl
from jax.experimental.pallas import tpu as pltpu
from jax.sharding import PartitionSpec as P

MESH = pl.DeviceIdType.MESH
F32 = jnp.float32
BF16 = jnp.bfloat16
I32 = jnp.int32
PLACE, WHICH, TARGET, PAIR, COLUMN = 0, 32, 48, 64, 80
BEHIND = 3
BEHIND_FIRST = 6


def kernel(
    a_cols_hbm, p_cols_hbm, c_cols_hbm, a_hbm, p_hbm, out_v,
    a_own, a_far, p_own, p_turn, band, begun, spreadable, placed, window, outer, inner,
    from_outer, from_inner, center, gathered, terms, terms_in, sums, sums_in, p_cols_v, c_cols_v, far_cols_v, tab_v, tab, own_cols, far_cols,
    load_sem, a_send, a_recv, c_send, c_recv, p_send, p_recv, s_send, s_recv, g_send, g_recv, t_send, t_recv, gate,
):
    grp = lax.axis_index("grp")
    row = lax.axis_index("row")
    n_row = lax.axis_size("row")
    core = lax.rem(row, 2)
    half = lax.rem(grp, 2)

    def along_row(by):
        return (grp, lax.rem(row + by + n_row, n_row))

    def along_grp(by):
        return (lax.rem(grp + by, 4), row)

    partner = (jnp.where(core == 0, grp + 1 - 2 * half, 3 - grp), row)
    sibling = (grp, row + 1 - 2 * core)
    outside = along_row(2 * core - 1)

    def remote(src, dst, send, recv, device):
        return pltpu.make_async_remote_copy(
            src_ref=src, dst_ref=dst, send_sem=send, recv_sem=recv, device_id=device, device_id_type=MESH
        )

    load_p = pltpu.make_async_copy(p_hbm, p_own, load_sem.at[0])
    load_p_cols = pltpu.make_async_copy(p_cols_hbm, p_cols_v.at[:, pl.ds(128, 1024)], load_sem.at[1])
    load_c_cols = pltpu.make_async_copy(c_cols_hbm, c_cols_v.at[:, pl.ds(128, 512)], load_sem.at[2])
    load_a = pltpu.make_async_copy(a_hbm, a_own, load_sem.at[3])
    load_own_cols = pltpu.make_async_copy(a_cols_hbm, own_cols, load_sem.at[4])
    for load in (load_p, load_p_cols, load_c_cols, load_a, load_own_cols):
        load.start()

    place_z = lax.rem(row // 2, 16)
    below = row >= 2
    above = row < n_row - 2
    first = (place_z == 0) & below
    last = (place_z == 15) & above
    has_outer = jnp.where(core == 0, row, n_row - 1 - row) >= 2

    barrier = pltpu.get_barrier_semaphore()

    def signal(semaphore, peer):
        pl.semaphore_signal(semaphore, inc=1, device_id=peer, device_id_type=MESH)

    for by in (1, 2, 3):
        signal(barrier, along_grp(by))
    signal(barrier, sibling)

    @pl.when(below)
    def _():
        signal(barrier, along_row(-2))

    @pl.when(below & (core == 0))
    def _():
        signal(barrier, along_row(-1))

    @pl.when(above & jnp.logical_not(last))
    def _():
        signal(barrier, along_row(2))

    @pl.when(above & jnp.logical_not(last) & (core == 1))
    def _():
        signal(barrier, along_row(1))


    lane = lax.broadcasted_iota(I32, (1, 128), 1)

    def from_lane(ref, start):
        begin = start + 128
        tile = begin // 128
        shift = lax.rem(begin, 128)
        first = pltpu.roll(ref[:, pl.ds(pl.multiple_of(tile * 128, 128), 128)], 128 - shift, 1)
        second = pltpu.roll(ref[:, pl.ds(pl.multiple_of(tile * 128 + 128, 128), 128)], 128 - shift, 1)
        return jnp.where(lane < 128 - shift, first, second)

    load_p_cols.wait()
    load_c_cols.wait()
    band_cols = from_lane(p_cols_v, row * 8 - 16)
    sub = lax.broadcasted_iota(I32, (32, 128), 0)
    place = jnp.full((32, 128), 4, I32)
    which = jnp.full((16, 128), 4, I32)
    pair = jnp.full((16, 128), 160, I32)
    for p in range(4):
        cols = band_cols[p : p + 1]
        column = cols - (row - 3) * 4
        place = jnp.where(column == sub, p, place)
        which = jnp.where(cols - (row - 1) * 4 == sub[:16], p, which)
        pair = jnp.where((column == 2 * sub[:16]) | (column == 2 * sub[:16] + 1), 4 * lane + p, pair)
    columns = jnp.clip(band_cols - (row - 3) * 4, 0, 27)
    target = from_lane(c_cols_v, row * 4 - 4) - (row - 3) * 4
    tab_v[PLACE : PLACE + 32] = place
    tab_v[PAIR : PAIR + 16] = pair
    tab_v[COLUMN : COLUMN + 4] = columns - (columns & 1)
    tab_v[WHICH : WHICH + 16] = which
    tab_v[TARGET : TARGET + 16] = jnp.where((target >= 0) & (target < 28), target, 28)

    left = lax.broadcasted_iota(I32, (128, 128), 1) < 64
    left16 = lax.broadcasted_iota(jnp.int16, (128, 128), 1) < 64

    def turn(x):
        return pltpu.roll(x.astype(F32), 64, 1).astype(x.dtype)

    load_p.wait()

    def halve(i, carry):
        for pair in range(2):
            x, y = p_own[i, 2 * pair], p_own[i, 2 * pair + 1]
            x_turned, y_turned = turn(x), turn(y)
            band[2, i, pair] = jnp.where(half == 0, jnp.where(left, x, y_turned), jnp.where(left, x_turned, y))
        return carry

    lax.fori_loop(0, 8, halve, 0)

    pl.semaphore_wait(barrier, 4 + jnp.where(above, 1 + core, 0) + jnp.where(below & jnp.logical_not(first), 2 - core, 0))

    @pl.when(last & (core == 1))
    def _():
        signal(gate, along_row(1))

    @pl.when(last)
    def _():
        signal(gate, along_row(2))


    def a_copy(i):
        return remote(a_hbm.at[i], a_far.at[i], a_send.at[i], a_recv.at[i], partner)

    def last_copy(part):
        slots = pl.ds(5 * part, 5 - 3 * part)
        return remote(a_hbm.at[7, slots], a_far.at[7, slots], a_send.at[7 + part], a_recv.at[7 + part], partner)

    cols_copy = remote(a_cols_hbm, far_cols_v, c_send, c_recv, partner)
    cols_copy.start()
    for i in range(7):
        a_copy(i).start()
    for part in range(2):
        last_copy(part).start()

    near = 3 - 2 * core

    def p_copy(kind, src, dst, n, device):
        return remote(band.at[src, n], band.at[dst, n], p_send.at[kind, n], p_recv.at[dst, n], device)

    def p_next(n):
        return p_copy(0, 2, 0, n, along_row(2))

    def p_prev(n):
        return p_copy(1, 2, 4, n, along_row(-2))

    def p_sibling(n):
        return p_copy(2, 2, 4 - near, n, sibling)

    def p_pass(n):
        return p_copy(3, 4 - 4 * core, near, n, sibling)

    def start_all(copy):
        def one(n, carry):
            copy(n).start()
            return carry

        lax.fori_loop(0, 8, one, 0)

    @pl.when(above & (core == 1))
    def _():
        start_all(p_next)

    @pl.when(below & jnp.logical_not(first) & (core == 0))
    def _():
        start_all(p_prev)

    start_all(p_sibling)

    to_smem = pltpu.make_async_copy(tab_v, tab, load_sem.at[5])
    to_smem.start()

    def transpose(i, carry):
        for q in range(4):
            p_turn[i, q] = p_own[i, q].T
        p_turn[i, 4] = jnp.zeros((128, 128), BF16)
        window[i, 28] = jnp.zeros((128, 128), BF16)
        return carry

    lax.fori_loop(0, 8, transpose, 0)
    spreadable[4] = jnp.zeros((128, 128), BF16)
    placed[160] = jnp.zeros((128, 128), BF16)
    to_smem.wait()

    def place_lines(slot, begin, count):
        def one(n, carry):
            line = slot * 8 + n
            for pair in range(2):
                x = band[slot, n, pair]
                turned = turn(x)
                spreadable[2 * pair] = jnp.where(left16, x, turned)
                spreadable[2 * pair + 1] = jnp.where(left16, turned, x)
            for p in range(4):
                column = tab[COLUMN + p, line]
                before = spreadable[tab[PLACE + column, line]]
                after = spreadable[tab[PLACE + 1 + column, line]]
                placed[4 * line + p] = jnp.where(left16, before, after)
            return carry

        lax.fori_loop(begin, begin + count, one, 0)

    def arrived(slot, n):
        p_copy(0, slot, slot, n, sibling).wait_recv()

    def there(slot):
        return jnp.where(slot > 2, above, below)

    def take(slot, n):
        @pl.when(there(slot))
        def _():
            arrived(slot, n)

            @pl.when(slot == 4 - 4 * core)
            def _():
                p_pass(n).start()

            place_lines(slot, n, 1)

    def follow(slot, n):
        @pl.when((n >= 0) & (slot == 4 - near) & there(slot))
        def _():
            arrived(slot, n)
            place_lines(slot, n, 1)

    place_lines(2, 0, 8)
    for n in range(8):
        arrived(near, n)
    place_lines(near, 0, 8)

    cols_copy.wait_recv()
    far_to_smem = pltpu.make_async_copy(far_cols_v, far_cols, load_sem.at[6])
    far_to_smem.start()
    load_own_cols.wait()
    load_a.wait()
    far_to_smem.wait()
    first_line = row * 8 - 16

    def tile_maker(i, slots):
        lhs = jnp.concatenate([(a_own if s < 7 else a_far)[i, s % 7] for s in slots], axis=1)
        lines = [(own_cols if s < 7 else far_cols)[s % 7, 0, i] - first_line for s in slots]
        lines = [jnp.clip(line, 0, 39) for line in lines]

        def tile(n):
            rhs = jnp.concatenate(
                [
                    jnp.concatenate([placed[tab[PAIR + 2 * n + u, line]] for line in lines], axis=0)
                    for u in range(2)
                ],
                axis=1,
            )
            return jnp.dot(lhs, rhs, preferred_element_type=F32)

        return tile

    def split(i, n, acc):
        for u in range(2):
            value = acc[:, u * 128 : (u + 1) * 128]
            high = value.astype(BF16).astype(F32)
            low = value - high
            window[i, 4 * n + 2 * u] = jnp.where(left, high, pltpu.roll(low, 64, 1)).astype(BF16)
            window[i, 4 * n + 2 * u + 1] = jnp.where(left, pltpu.roll(high, 64, 1), low).astype(BF16)

    def fine_row(i, begin, count):
        tile = tile_maker(i, range(14))
        for n in [begin + k for k in range(count)]:
            split(i, n, tile(n))

    def last_row():
        last_copy(0).wait_recv()
        tile = tile_maker(7, range(12))
        for n in range(7):
            begun[n] = tile(n)
        last_copy(1).wait_recv()
        tile = tile_maker(7, range(12, 14))
        for n in range(7):
            split(7, n, begun[n] + tile(n))

    ahead = first & (core == 0)
    late_near = last & (core == 0)
    late_follow = last & (core == 1)
    late_take = first & (core == 1)

    def follow_all(n, carry):
        follow(4 - near, n)

        @pl.when((n == 3) & late_near)
        def _():
            start_all(p_next)

        return carry

    def take_near(n, carry):
        take(4 - 4 * core, n)

        @pl.when(jnp.logical_not(ahead | last))
        def _():
            follow(4 - near, n - 2)

        @pl.when(late_take)
        def _():
            take(4 * core, n)

        @pl.when((n == 5) & above & (core == 0) & jnp.logical_not(last))
        def _():
            start_all(p_next)

        @pl.when((n == 5) & below & (core == 1))
        def _():
            @pl.when(first)
            def _():
                pl.semaphore_wait(gate, 1)

            start_all(p_prev)

        return carry

    def take_far(n, carry):
        take(4 * core, n)
        return carry

    def four_tiles(i, carry):
        a_copy(2 * i).wait_recv()
        a_copy(2 * i + 1).wait_recv()
        fine_row(2 * i, 3 - 3 * core, 4)
        fine_row(2 * i + 1, 3 - 3 * core, 4)
        return carry

    def other_three_tiles(i, carry):
        fine_row(2 * i, 4 * core, 3)
        fine_row(2 * i + 1, 4 * core, 3)
        return carry

    def three_tiles(i, carry):
        a_copy(2 * i).wait_recv()
        a_copy(2 * i + 1).wait_recv()
        fine_row(2 * i, 0, 3)
        fine_row(2 * i + 1, 0, 3)
        return carry

    def other_four_tiles(i, carry):
        fine_row(2 * i, 3, 4)
        fine_row(2 * i + 1, 3, 4)
        return carry

    def two_rows(i, carry):
        a_copy(2 * i).wait_recv()
        a_copy(2 * i + 1).wait_recv()
        fine_row(2 * i, 0, 7)
        fine_row(2 * i + 1, 0, 7)
        return carry

    def whole_row(i, carry):
        a_copy(i).wait_recv()
        fine_row(i, 0, 7)
        return carry

    @pl.when(late_near)
    def _():
        lax.fori_loop(0, 8, follow_all, 0)

    lax.fori_loop(0, 8, take_near, 0)

    @pl.when(ahead)
    def _():
        pl.semaphore_wait(gate, 2)
        start_all(p_prev)
        lax.fori_loop(0, 8, follow_all, 0)

    @pl.when(jnp.logical_not(ahead | last))
    def _():
        follow(4 - near, 6)
        follow(4 - near, 7)

    pairs = jnp.where(ahead, 3, 2)

    @pl.when(late_follow)
    def _():
        lax.fori_loop(0, 2, three_tiles, 0)
        lax.fori_loop(0, 8, follow_all, 0)
        lax.fori_loop(0, 8, take_far, 0)
        lax.fori_loop(0, 2, other_four_tiles, 0)

    @pl.when(jnp.logical_not(late_follow))
    def _():
        lax.fori_loop(0, pairs, four_tiles, 0)
        lax.fori_loop(jnp.where(late_take, 8, 0), 8, take_far, 0)
        lax.fori_loop(0, pairs, other_three_tiles, 0)

    lax.fori_loop(pairs, 3, two_rows, 0)

    whole_row(6, 0)

    @pl.when(jnp.logical_not(last))
    def _():
        last_row()

    @pl.when(last)
    def _():
        last_copy(0).wait_recv()
        last_copy(1).wait_recv()
        fine_row(7, 0, 7)

    def unit(n):
        early = n < 12
        return jnp.where(early, n // 3, n - 12), jnp.where(early, lax.rem(n, 3), 3)

    def steps(t):
        return jnp.where(t == 0, 2, jnp.where(t == 1, 1, jnp.where(t == 2, 3, 0)))

    def coarse_tiles(c, t):
        lhs = jnp.concatenate([p_turn[i, tab[WHICH + c, 16 + i]] for i in range(8)], axis=1)
        k = TARGET + lax.rem(grp + steps(t), 4) * 4
        tiles = []
        for pair in range(2):
            first = tab[k + 2 * pair, c]
            second = tab[k + 2 * pair + 1, c]
            rhs = jnp.concatenate(
                [jnp.concatenate([window[i, first], window[i, second]], axis=1) for i in range(8)], axis=0
            )
            acc = jnp.dot(lhs, rhs, preferred_element_type=F32)
            x, y = acc[:, :128], acc[:, 128:]
            tiles.append(jnp.where(left, x, y) + pltpu.roll(jnp.where(left, y, x), 64, 1))
        return tiles

    def outer_copy(n):
        return remote(outer.at[n], from_outer.at[n], s_send.at[0, n], s_recv.at[0, n], outside)

    sums_first = last & (core == 1)
    gets_sums = first & (core == 0)

    def by_sums(n):
        return unit(n)[0] == 0

    def sends_outer(n):
        return has_outer & jnp.logical_not(sums_first & by_sums(n))

    def gets_outer(n):
        return has_outer & jnp.logical_not(gets_sums & by_sums(n))

    def term_copy(t):
        return remote(terms.at[t], terms_in.at[t], t_send.at[t], t_recv.at[t], along_grp(steps(t)))

    def sums_copy():
        return remote(sums, sums_in, t_send.at[3], t_recv.at[3], outside)

    def whole_tiles(own, from_two, from_one, from_three):
        same = own + from_two
        other = from_one + from_three
        x = jnp.where(half == 0, same, other)
        y = jnp.where(half == 0, other, same)
        return jnp.where(left, x, pltpu.roll(y, 64, 1)), jnp.where(left, pltpu.roll(x, 64, 1), y)

    def inner_copy(n):
        return remote(inner.at[n], from_inner.at[n], s_send.at[1, n], s_recv.at[1, n], sibling)

    def group_copy(c, t):
        return remote(
            center.at[3 * c + t], gathered.at[t, c], g_send.at[t, c], g_recv.at[t, c], along_grp(steps(t))
        )

    def fill(ref, n, c, t):
        for pair, tile in enumerate(coarse_tiles(c, t)):
            ref[n, pair] = tile

    def absorb(n):
        inner_copy(n).wait_recv()

        @pl.when(gets_outer(n))
        def _():
            outer_copy(n).wait_recv()

        center[n] = center[n] + (from_inner[n] + jnp.where(gets_outer(n), from_outer[n], 0.0))

    behind = jnp.where(first & (core == 0), BEHIND_FIRST, BEHIND)

    def sum_first(n):
        @pl.when(n < 4)
        def _():
            fill(terms, n, 8, n)

        @pl.when((n > 0) & (n < 4))
        def _():
            term_copy(n - 1).start()

        @pl.when(n == 8)
        def _():
            for t in range(3):
                term_copy(t).wait_recv()
            for pair in range(2):
                tiles = whole_tiles(terms[3, pair], terms_in[0, pair], terms_in[1, pair], terms_in[2, pair])
                sums[2 * pair], sums[2 * pair + 1] = tiles

        @pl.when(n == 9)
        def _():
            sums_copy().start()

    def one_unit(n, carry):
        c, t = unit(n)

        soon = gets_sums & (n >= 2) & (n < 5)
        done = jnp.where(soon, n - 2, n - behind)
        taken = (n >= behind + jnp.where(gets_sums, 3, 0)) | soon

        @pl.when(taken)
        def _():
            absorb(done)

        m = jnp.where(sums_first, jnp.where(n < 9, n + 3, jnp.where(n < 12, n + 4, 0)), n)
        outer_c, outer_t = unit(m)
        fill(outer, m, outer_c + 8 * core, outer_t)

        @pl.when(taken & (done < 12))
        def _():
            done_c, done_t = unit(done)
            group_copy(done_c, done_t).start()

        @pl.when(has_outer & jnp.logical_not(sums_first & (n >= 12)))
        def _():
            outer_copy(m).start()

        fill(inner, n, c + 8 - 8 * core, t)
        inner_copy(n).start()
        fill(center, n, c + 4, t)

        @pl.when(sums_first)
        def _():
            sum_first(n)

        return carry

    lax.fori_loop(0, 16, one_unit, 0)

    cols_copy.wait_send()
    for i in range(7):
        a_copy(i).wait_send()
    for part in range(2):
        last_copy(part).wait_send()
    for n in range(8):
        p_sibling(n).wait_send()

        @pl.when(above)
        def _():
            p_next(n).wait_send()

        @pl.when(below)
        def _():
            p_prev(n).wait_send()

        @pl.when(there(4 - 4 * core))
        def _():
            p_pass(n).wait_send()

    def finish(c):
        for t in range(3):
            group_copy(c, t).wait_recv()
        for pair in range(2):
            tiles = whole_tiles(
                center[12 + c, pair], gathered[0, c, pair], gathered[1, c, pair], gathered[2, c, pair]
            )
            out_v[c, 2 * pair], out_v[c, 2 * pair + 1] = tiles

    def absorb_rest(n, carry):
        absorb(n)

        @pl.when((n > 16 - behind) & (n < 13))
        def _():
            done_c, done_t = unit(n - 1)
            group_copy(done_c, done_t).start()

        @pl.when(n >= 13)
        def _():
            finish(n - 13)

        return carry

    lax.fori_loop(16 - behind, 15, absorb_rest, 0)
    finish(2)

    def sent(n, carry):
        inner_copy(n).wait_send()

        @pl.when(sends_outer(n))
        def _():
            outer_copy(n).wait_send()

        @pl.when(n < 9)
        def _():
            group_copy(n // 3, lax.rem(n, 3)).wait_send()

        return carry

    lax.fori_loop(0, 15, sent, 0)
    absorb(15)
    finish(3)

    @pl.when(gets_sums)
    def _():
        sums_copy().wait_recv()
        out_v[0] = out_v[0] + sums_in[...]

    @pl.when(sums_first)
    def _():
        for t in range(3):
            term_copy(t).wait_send()
        sums_copy().wait_send()

    sent(15, 0)
    for t in range(3):
        group_copy(3, t).wait_send()


def body(a_tiles, a_cols, p_tiles, p_cols, c_cols):
    operands = (a_cols.transpose(2, 1, 0), p_cols.T, c_cols.T, a_tiles.reshape(8, 7, 128, 128), p_tiles)
    dma = pltpu.SemaphoreType.DMA
    anywhere = pl.BlockSpec(memory_space=pl.ANY)
    side = pltpu.VMEM((16, 2, 128, 128), F32)
    return pl.pallas_call(
        kernel,
        out_shape=pltpu.VMEM((4, 4, 128, 128), F32),
        in_specs=[anywhere] * 5,
        out_specs=pl.BlockSpec(memory_space=pltpu.VMEM),
        scratch_shapes=[
            pltpu.VMEM((8, 7, 128, 128), BF16),
            pltpu.VMEM((8, 7, 128, 128), BF16),
            pltpu.VMEM((8, 4, 128, 128), BF16),
            pltpu.VMEM((8, 5, 128, 128), BF16),
            pltpu.VMEM((5, 8, 2, 128, 128), BF16),
            pltpu.VMEM((7, 128, 256), F32),
            pltpu.VMEM((5, 128, 128), BF16),
            pltpu.VMEM((161, 128, 128), BF16),
            pltpu.VMEM((8, 29, 128, 128), BF16),
            side,
            side,
            side,
            side,
            side,
            pltpu.VMEM((3, 4, 2, 128, 128), F32),
            pltpu.VMEM((4, 2, 128, 128), F32),
            pltpu.VMEM((3, 2, 128, 128), F32),
            pltpu.VMEM((4, 128, 128), F32),
            pltpu.VMEM((4, 128, 128), F32),
            pltpu.VMEM((4, 1280), I32),
            pltpu.VMEM((16, 768), I32),
            pltpu.VMEM((7, 1, 8), I32),
            pltpu.VMEM((88, 128), I32),
            pltpu.SMEM((88, 128), I32),
            pltpu.SMEM((7, 1, 8), I32),
            pltpu.SMEM((7, 1, 8), I32),
            dma((7,)),
            dma((9,)),
            dma((9,)),
            dma,
            dma,
            dma((4, 8)),
            dma((5, 8)),
            dma((2, 16)),
            dma((2, 16)),
            dma((3, 4)),
            dma((3, 4)),
            dma((4,)),
            dma((4,)),
            pltpu.SemaphoreType.REGULAR,
        ],
        compiler_params=pltpu.CompilerParams(
            collective_id=0, has_side_effects=True, vmem_limit_bytes=52 * 1024 * 1024
        ),
        cost_estimate=pl.CostEstimate(flops=4_000_000_000, bytes_accessed=8_000_000, transcendentals=0),
    )(*[pltpu.with_memory_space_constraint(x, pltpu.HBM) for x in operands])


def solution(mesh):
    return jax.shard_map(
        body,
        mesh=mesh,
        in_specs=(
            P("row", "grp", None, None, None),
            P("row", "grp", None),
            P("row", None, None, None),
            P(),
            P(),
        ),
        out_specs=P("row", "grp", None, None),
        check_vma=False,
    )
```

```python
import jax
import jax.numpy as jnp
from jax import lax
from jax.experimental import pallas as pl
from jax.experimental.pallas import tpu as pltpu
from jax.sharding import PartitionSpec as P

MESH = pl.DeviceIdType.MESH
F32 = jnp.float32
BF16 = jnp.bfloat16
I32 = jnp.int32
PLACE, WHICH, TARGET, PAIR, COLUMN = 0, 32, 48, 64, 80
BEHIND = 3
BEHIND_FIRST = 7


def kernel(
    a_cols_hbm, p_cols_hbm, c_cols_hbm, a_hbm, p_hbm, out_v,
    a_own, a_far, p_own, p_turn, band, begun, spreadable, placed, window, outer, inner,
    from_outer, from_inner, center, gathered, terms, terms_in, sums, sums_in, p_cols_v, c_cols_v, far_cols_v, tab_v, tab, own_cols, far_cols,
    load_sem, a_send, a_recv, c_send, c_recv, p_send, p_recv, s_send, s_recv, g_send, g_recv, t_send, t_recv, gate,
):
    grp = lax.axis_index("grp")
    row = lax.axis_index("row")
    n_row = lax.axis_size("row")
    core = lax.rem(row, 2)
    half = lax.rem(grp, 2)

    def along_row(by):
        return (grp, lax.rem(row + by + n_row, n_row))

    def along_grp(by):
        return (lax.rem(grp + by, 4), row)

    partner = (jnp.where(core == 0, grp + 1 - 2 * half, 3 - grp), row)
    sibling = (grp, row + 1 - 2 * core)
    outside = along_row(2 * core - 1)

    def remote(src, dst, send, recv, device):
        return pltpu.make_async_remote_copy(
            src_ref=src, dst_ref=dst, send_sem=send, recv_sem=recv, device_id=device, device_id_type=MESH
        )

    load_p = pltpu.make_async_copy(p_hbm, p_own, load_sem.at[0])
    load_p_cols = pltpu.make_async_copy(p_cols_hbm, p_cols_v.at[:, pl.ds(128, 1024)], load_sem.at[1])
    load_c_cols = pltpu.make_async_copy(c_cols_hbm, c_cols_v.at[:, pl.ds(128, 512)], load_sem.at[2])
    load_a = pltpu.make_async_copy(a_hbm, a_own, load_sem.at[3])
    load_own_cols = pltpu.make_async_copy(a_cols_hbm, own_cols, load_sem.at[4])
    for load in (load_p, load_p_cols, load_c_cols, load_a, load_own_cols):
        load.start()

    place_z = lax.rem(row // 2, 16)
    below = row >= 2
    above = row < n_row - 2
    first = (place_z == 0) & below
    last = (place_z == 15) & above
    has_outer = jnp.where(core == 0, row, n_row - 1 - row) >= 2

    barrier = pltpu.get_barrier_semaphore()

    def signal(semaphore, peer):
        pl.semaphore_signal(semaphore, inc=1, device_id=peer, device_id_type=MESH)

    for by in (1, 2, 3):
        signal(barrier, along_grp(by))
    signal(barrier, sibling)

    @pl.when(below)
    def _():
        signal(barrier, along_row(-2))

    @pl.when(below & (core == 0))
    def _():
        signal(barrier, along_row(-1))

    @pl.when(above & jnp.logical_not(last))
    def _():
        signal(barrier, along_row(2))

    @pl.when(above & jnp.logical_not(last) & (core == 1))
    def _():
        signal(barrier, along_row(1))


    lane = lax.broadcasted_iota(I32, (1, 128), 1)

    def from_lane(ref, start):
        begin = start + 128
        tile = begin // 128
        shift = lax.rem(begin, 128)
        first = pltpu.roll(ref[:, pl.ds(pl.multiple_of(tile * 128, 128), 128)], 128 - shift, 1)
        second = pltpu.roll(ref[:, pl.ds(pl.multiple_of(tile * 128 + 128, 128), 128)], 128 - shift, 1)
        return jnp.where(lane < 128 - shift, first, second)

    left = lax.broadcasted_iota(I32, (128, 128), 1) < 64
    left16 = lax.broadcasted_iota(jnp.int16, (128, 128), 1) < 64

    def turn(x):
        return pltpu.roll(x.astype(F32), 64, 1).astype(x.dtype)

    def prepare():
        load_p_cols.wait()
        load_c_cols.wait()
        band_cols = from_lane(p_cols_v, row * 8 - 16)
        sub = lax.broadcasted_iota(I32, (32, 128), 0)
        place = jnp.full((32, 128), 4, I32)
        which = jnp.full((16, 128), 4, I32)
        pair = jnp.full((16, 128), 160, I32)
        for p in range(4):
            cols = band_cols[p : p + 1]
            column = cols - (row - 3) * 4
            place = jnp.where(column == sub, p, place)
            which = jnp.where(cols - (row - 1) * 4 == sub[:16], p, which)
            pair = jnp.where((column == 2 * sub[:16]) | (column == 2 * sub[:16] + 1), 4 * lane + p, pair)
        columns = jnp.clip(band_cols - (row - 3) * 4, 0, 27)
        target = from_lane(c_cols_v, row * 4 - 4) - (row - 3) * 4
        tab_v[PLACE : PLACE + 32] = place
        tab_v[PAIR : PAIR + 16] = pair
        tab_v[COLUMN : COLUMN + 4] = columns - (columns & 1)
        tab_v[WHICH : WHICH + 16] = which
        tab_v[TARGET : TARGET + 16] = jnp.where((target >= 0) & (target < 28), target, 28)

        load_p.wait()

        def halve(i, carry):
            for pair in range(2):
                x, y = p_own[i, 2 * pair], p_own[i, 2 * pair + 1]
                x_turned, y_turned = turn(x), turn(y)
                band[2, i, pair] = jnp.where(half == 0, jnp.where(left, x, y_turned), jnp.where(left, x_turned, y))
            return carry

        lax.fori_loop(0, 8, halve, 0)

    early = (grp < 2) | (place_z < 8)

    @pl.when(early)
    def _():
        prepare()

    pl.semaphore_wait(barrier, 4 + jnp.where(above, 1 + core, 0) + jnp.where(below & jnp.logical_not(first), 2 - core, 0))

    @pl.when(last & (core == 1))
    def _():
        signal(gate, along_row(1))

    @pl.when(last)
    def _():
        signal(gate, along_row(2))


    def a_copy(i):
        return remote(a_hbm.at[i], a_far.at[i], a_send.at[i], a_recv.at[i], partner)

    def last_copy(part):
        slots = pl.ds(5 * part, 5 - 3 * part)
        return remote(a_hbm.at[7, slots], a_far.at[7, slots], a_send.at[7 + part], a_recv.at[7 + part], partner)

    cols_copy = remote(a_cols_hbm, far_cols_v, c_send, c_recv, partner)
    cols_copy.start()
    for i in range(7):
        a_copy(i).start()
    for part in range(2):
        last_copy(part).start()

    @pl.when(jnp.logical_not(early))
    def _():
        prepare()

    near = 3 - 2 * core

    def p_copy(kind, src, dst, n, device):
        return remote(band.at[src, n], band.at[dst, n], p_send.at[kind, n], p_recv.at[dst, n], device)

    def p_next(n):
        return p_copy(0, 2, 0, n, along_row(2))

    def p_prev(n):
        return p_copy(1, 2, 4, n, along_row(-2))

    def p_sibling(n):
        return p_copy(2, 2, 4 - near, n, sibling)

    def p_pass(n):
        return p_copy(3, 4 - 4 * core, near, n, sibling)

    def start_all(copy):
        def one(n, carry):
            copy(n).start()
            return carry

        lax.fori_loop(0, 8, one, 0)

    @pl.when(above & (core == 1))
    def _():
        start_all(p_next)

    @pl.when(below & jnp.logical_not(first) & (core == 0))
    def _():
        start_all(p_prev)

    start_all(p_sibling)

    to_smem = pltpu.make_async_copy(tab_v, tab, load_sem.at[5])
    to_smem.start()

    def transpose(i, carry):
        for q in range(4):
            p_turn[i, q] = p_own[i, q].T
        p_turn[i, 4] = jnp.zeros((128, 128), BF16)
        window[i, 28] = jnp.zeros((128, 128), BF16)
        return carry

    lax.fori_loop(0, 8, transpose, 0)
    spreadable[4] = jnp.zeros((128, 128), BF16)
    placed[160] = jnp.zeros((128, 128), BF16)
    to_smem.wait()

    def place_lines(slot, begin, count):
        def one(n, carry):
            line = slot * 8 + n
            for pair in range(2):
                x = band[slot, n, pair]
                turned = turn(x)
                spreadable[2 * pair] = jnp.where(left16, x, turned)
                spreadable[2 * pair + 1] = jnp.where(left16, turned, x)
            for p in range(4):
                column = tab[COLUMN + p, line]
                before = spreadable[tab[PLACE + column, line]]
                after = spreadable[tab[PLACE + 1 + column, line]]
                placed[4 * line + p] = jnp.where(left16, before, after)
            return carry

        lax.fori_loop(begin, begin + count, one, 0)

    def arrived(slot, n):
        p_copy(0, slot, slot, n, sibling).wait_recv()

    def there(slot):
        return jnp.where(slot > 2, above, below)

    def take(slot, n):
        @pl.when(there(slot))
        def _():
            arrived(slot, n)

            @pl.when(slot == 4 - 4 * core)
            def _():
                p_pass(n).start()

            place_lines(slot, n, 1)

    def follow(slot, n):
        @pl.when((n >= 0) & (slot == 4 - near) & there(slot))
        def _():
            arrived(slot, n)
            place_lines(slot, n, 1)

    place_lines(2, 0, 8)
    for n in range(8):
        arrived(near, n)
    place_lines(near, 0, 8)

    cols_copy.wait_recv()
    far_to_smem = pltpu.make_async_copy(far_cols_v, far_cols, load_sem.at[6])
    far_to_smem.start()
    load_own_cols.wait()
    load_a.wait()
    far_to_smem.wait()
    first_line = row * 8 - 16

    def tile_maker(i, slots):
        lhs = jnp.concatenate([(a_own if s < 7 else a_far)[i, s % 7] for s in slots], axis=1)
        lines = [(own_cols if s < 7 else far_cols)[s % 7, 0, i] - first_line for s in slots]
        lines = [jnp.clip(line, 0, 39) for line in lines]

        def tile(n):
            rhs = jnp.concatenate(
                [
                    jnp.concatenate([placed[tab[PAIR + 2 * n + u, line]] for line in lines], axis=0)
                    for u in range(2)
                ],
                axis=1,
            )
            return jnp.dot(lhs, rhs, preferred_element_type=F32)

        return tile

    def split(i, n, acc):
        for u in range(2):
            value = acc[:, u * 128 : (u + 1) * 128]
            high = value.astype(BF16).astype(F32)
            low = value - high
            window[i, 4 * n + 2 * u] = jnp.where(left, high, pltpu.roll(low, 64, 1)).astype(BF16)
            window[i, 4 * n + 2 * u + 1] = jnp.where(left, pltpu.roll(high, 64, 1), low).astype(BF16)

    def fine_row(i, begin, count):
        tile = tile_maker(i, range(14))
        for n in [begin + k for k in range(count)]:
            split(i, n, tile(n))

    def last_row():
        last_copy(0).wait_recv()
        tile = tile_maker(7, range(12))
        for n in range(7):
            begun[n] = tile(n)
        last_copy(1).wait_recv()
        tile = tile_maker(7, range(12, 14))
        for n in range(7):
            split(7, n, begun[n] + tile(n))

    ahead = first & (core == 0)
    late_near = last & (core == 0)
    late_follow = last & (core == 1)
    late_take = first & (core == 1)

    def follow_all(n, carry):
        follow(4 - near, n)

        @pl.when((n == 1) & late_near)
        def _():
            start_all(p_next)

        return carry

    def take_near(n, carry):
        take(4 - 4 * core, n)

        @pl.when(jnp.logical_not(ahead | last))
        def _():
            follow(4 - near, n - 2)

        @pl.when(late_take)
        def _():
            take(4 * core, n)

        @pl.when((n == 5) & above & (core == 0) & jnp.logical_not(last))
        def _():
            start_all(p_next)

        @pl.when((n == jnp.where(first, 3, 5)) & below & (core == 1))
        def _():
            @pl.when(first)
            def _():
                pl.semaphore_wait(gate, 1)

            start_all(p_prev)

        return carry

    def take_far(n, carry):
        take(4 * core, n)
        return carry

    def four_tiles(i, carry):
        a_copy(2 * i).wait_recv()
        a_copy(2 * i + 1).wait_recv()
        fine_row(2 * i, 3 - 3 * core, 4)
        fine_row(2 * i + 1, 3 - 3 * core, 4)
        return carry

    def other_three_tiles(i, carry):
        fine_row(2 * i, 4 * core, 3)
        fine_row(2 * i + 1, 4 * core, 3)
        return carry

    def three_tiles(i, carry):
        a_copy(2 * i).wait_recv()
        a_copy(2 * i + 1).wait_recv()
        fine_row(2 * i, 0, 3)
        fine_row(2 * i + 1, 0, 3)
        return carry

    def other_four_tiles(i, carry):
        fine_row(2 * i, 3, 4)
        fine_row(2 * i + 1, 3, 4)
        return carry

    def two_rows(i, carry):
        a_copy(2 * i).wait_recv()
        a_copy(2 * i + 1).wait_recv()
        fine_row(2 * i, 0, 7)
        fine_row(2 * i + 1, 0, 7)
        return carry

    def whole_row(i, carry):
        a_copy(i).wait_recv()
        fine_row(i, 0, 7)
        return carry

    @pl.when(late_near)
    def _():
        lax.fori_loop(0, 8, follow_all, 0)

    lax.fori_loop(0, 8, take_near, 0)

    @pl.when(ahead)
    def _():
        pl.semaphore_wait(gate, 2)
        start_all(p_prev)
        lax.fori_loop(0, 8, follow_all, 0)

    @pl.when(jnp.logical_not(ahead | last))
    def _():
        follow(4 - near, 6)
        follow(4 - near, 7)

    pairs = jnp.where(ahead, 3, 2)

    @pl.when(late_follow)
    def _():
        lax.fori_loop(0, 2, three_tiles, 0)
        lax.fori_loop(0, 8, follow_all, 0)
        lax.fori_loop(0, 8, take_far, 0)
        lax.fori_loop(0, 2, other_four_tiles, 0)

    @pl.when(jnp.logical_not(late_follow))
    def _():
        lax.fori_loop(0, pairs, four_tiles, 0)
        lax.fori_loop(jnp.where(late_take, 8, 0), 8, take_far, 0)
        lax.fori_loop(0, pairs, other_three_tiles, 0)

    lax.fori_loop(pairs, 3, two_rows, 0)

    whole_row(6, 0)

    @pl.when(jnp.logical_not(last))
    def _():
        last_row()

    @pl.when(last)
    def _():
        last_copy(0).wait_recv()
        last_copy(1).wait_recv()
        fine_row(7, 0, 7)

    def unit(n):
        early = n < 12
        return jnp.where(early, n // 3, n - 12), jnp.where(early, lax.rem(n, 3), 3)

    def steps(t):
        return jnp.where(t == 0, 2, jnp.where(t == 1, 1, jnp.where(t == 2, 3, 0)))

    def coarse_tiles(c, t):
        lhs = jnp.concatenate([p_turn[i, tab[WHICH + c, 16 + i]] for i in range(8)], axis=1)
        k = TARGET + lax.rem(grp + steps(t), 4) * 4
        tiles = []
        for pair in range(2):
            first = tab[k + 2 * pair, c]
            second = tab[k + 2 * pair + 1, c]
            rhs = jnp.concatenate(
                [jnp.concatenate([window[i, first], window[i, second]], axis=1) for i in range(8)], axis=0
            )
            acc = jnp.dot(lhs, rhs, preferred_element_type=F32)
            x, y = acc[:, :128], acc[:, 128:]
            tiles.append(jnp.where(left, x, y) + pltpu.roll(jnp.where(left, y, x), 64, 1))
        return tiles

    def outer_copy(n):
        return remote(outer.at[n], from_outer.at[n], s_send.at[0, n], s_recv.at[0, n], outside)

    sums_first = last & (core == 1)
    gets_sums = first & (core == 0)

    def by_sums(n):
        return unit(n)[0] == 0

    def sends_outer(n):
        return has_outer & jnp.logical_not(sums_first & by_sums(n))

    def gets_outer(n):
        return has_outer & jnp.logical_not(gets_sums & by_sums(n))

    def term_copy(t):
        return remote(terms.at[t], terms_in.at[t], t_send.at[t], t_recv.at[t], along_grp(steps(t)))

    def sums_copy():
        return remote(sums, sums_in, t_send.at[3], t_recv.at[3], outside)

    def whole_tiles(own, from_two, from_one, from_three):
        same = own + from_two
        other = from_one + from_three
        x = jnp.where(half == 0, same, other)
        y = jnp.where(half == 0, other, same)
        return jnp.where(left, x, pltpu.roll(y, 64, 1)), jnp.where(left, pltpu.roll(x, 64, 1), y)

    def inner_copy(n):
        return remote(inner.at[n], from_inner.at[n], s_send.at[1, n], s_recv.at[1, n], sibling)

    def group_copy(c, t):
        return remote(
            center.at[3 * c + t], gathered.at[t, c], g_send.at[t, c], g_recv.at[t, c], along_grp(steps(t))
        )

    def fill(ref, n, c, t):
        for pair, tile in enumerate(coarse_tiles(c, t)):
            ref[n, pair] = tile

    def absorb(n):
        inner_copy(n).wait_recv()

        @pl.when(gets_outer(n))
        def _():
            outer_copy(n).wait_recv()

        center[n] = center[n] + (from_inner[n] + jnp.where(gets_outer(n), from_outer[n], 0.0))

    behind = jnp.where(first & (core == 0), BEHIND_FIRST, BEHIND)

    def sum_first(n):
        @pl.when(n < 4)
        def _():
            fill(terms, n, 8, n)

        @pl.when((n > 0) & (n < 4))
        def _():
            term_copy(n - 1).start()

        @pl.when(n == 8)
        def _():
            for t in range(3):
                term_copy(t).wait_recv()
            for pair in range(2):
                tiles = whole_tiles(terms[3, pair], terms_in[0, pair], terms_in[1, pair], terms_in[2, pair])
                sums[2 * pair], sums[2 * pair + 1] = tiles

        @pl.when(n == 9)
        def _():
            sums_copy().start()

    def one_unit(n, carry):
        c, t = unit(n)

        soon = gets_sums & (n >= 2) & (n < 5)
        done = jnp.where(soon, n - 2, n - behind)
        taken = (n >= behind + jnp.where(gets_sums, 3, 0)) | soon

        @pl.when(taken)
        def _():
            absorb(done)

        m = jnp.where(sums_first, jnp.where(n < 9, n + 3, jnp.where(n < 12, n + 4, 0)), n)
        outer_c, outer_t = unit(m)
        fill(outer, m, outer_c + 8 * core, outer_t)

        @pl.when(taken & (done < 12))
        def _():
            done_c, done_t = unit(done)
            group_copy(done_c, done_t).start()

        @pl.when(has_outer & jnp.logical_not(sums_first & (n >= 12)))
        def _():
            outer_copy(m).start()

        fill(inner, n, c + 8 - 8 * core, t)
        inner_copy(n).start()
        fill(center, n, c + 4, t)

        @pl.when(sums_first)
        def _():
            sum_first(n)

        return carry

    lax.fori_loop(0, 16, one_unit, 0)

    cols_copy.wait_send()
    for i in range(7):
        a_copy(i).wait_send()
    for part in range(2):
        last_copy(part).wait_send()
    for n in range(8):
        p_sibling(n).wait_send()

        @pl.when(above)
        def _():
            p_next(n).wait_send()

        @pl.when(below)
        def _():
            p_prev(n).wait_send()

        @pl.when(there(4 - 4 * core))
        def _():
            p_pass(n).wait_send()

    def finish(c):
        for t in range(3):
            group_copy(c, t).wait_recv()
        for pair in range(2):
            tiles = whole_tiles(
                center[12 + c, pair], gathered[0, c, pair], gathered[1, c, pair], gathered[2, c, pair]
            )
            out_v[c, 2 * pair], out_v[c, 2 * pair + 1] = tiles

    def absorb_rest(n, carry):
        absorb(n)

        @pl.when((n > 16 - behind) & (n < 13))
        def _():
            done_c, done_t = unit(n - 1)
            group_copy(done_c, done_t).start()

        @pl.when(n >= 13)
        def _():
            finish(n - 13)

        return carry

    lax.fori_loop(16 - behind, 15, absorb_rest, 0)
    finish(2)

    def sent(n, carry):
        inner_copy(n).wait_send()

        @pl.when(sends_outer(n))
        def _():
            outer_copy(n).wait_send()

        @pl.when(n < 9)
        def _():
            group_copy(n // 3, lax.rem(n, 3)).wait_send()

        return carry

    lax.fori_loop(0, 15, sent, 0)
    @pl.when(gets_sums)
    def _():
        sums_copy().wait_recv()
        out_v[0] = out_v[0] + sums_in[...]

    absorb(15)
    finish(3)

    @pl.when(sums_first)
    def _():
        for t in range(3):
            term_copy(t).wait_send()
        sums_copy().wait_send()

    sent(15, 0)
    for t in range(3):
        group_copy(3, t).wait_send()


def body(a_tiles, a_cols, p_tiles, p_cols, c_cols):
    operands = (a_cols.transpose(2, 1, 0), p_cols.T, c_cols.T, a_tiles.reshape(8, 7, 128, 128), p_tiles)
    dma = pltpu.SemaphoreType.DMA
    anywhere = pl.BlockSpec(memory_space=pl.ANY)
    side = pltpu.VMEM((16, 2, 128, 128), F32)
    return pl.pallas_call(
        kernel,
        out_shape=pltpu.VMEM((4, 4, 128, 128), F32),
        in_specs=[anywhere] * 5,
        out_specs=pl.BlockSpec(memory_space=pltpu.VMEM),
        scratch_shapes=[
            pltpu.VMEM((8, 7, 128, 128), BF16),
            pltpu.VMEM((8, 7, 128, 128), BF16),
            pltpu.VMEM((8, 4, 128, 128), BF16),
            pltpu.VMEM((8, 5, 128, 128), BF16),
            pltpu.VMEM((5, 8, 2, 128, 128), BF16),
            pltpu.VMEM((7, 128, 256), F32),
            pltpu.VMEM((5, 128, 128), BF16),
            pltpu.VMEM((161, 128, 128), BF16),
            pltpu.VMEM((8, 29, 128, 128), BF16),
            side,
            side,
            side,
            side,
            side,
            pltpu.VMEM((3, 4, 2, 128, 128), F32),
            pltpu.VMEM((4, 2, 128, 128), F32),
            pltpu.VMEM((3, 2, 128, 128), F32),
            pltpu.VMEM((4, 128, 128), F32),
            pltpu.VMEM((4, 128, 128), F32),
            pltpu.VMEM((4, 1280), I32),
            pltpu.VMEM((16, 768), I32),
            pltpu.VMEM((7, 1, 8), I32),
            pltpu.VMEM((88, 128), I32),
            pltpu.SMEM((88, 128), I32),
            pltpu.SMEM((7, 1, 8), I32),
            pltpu.SMEM((7, 1, 8), I32),
            dma((7,)),
            dma((9,)),
            dma((9,)),
            dma,
            dma,
            dma((4, 8)),
            dma((5, 8)),
            dma((2, 16)),
            dma((2, 16)),
            dma((3, 4)),
            dma((3, 4)),
            dma((4,)),
            dma((4,)),
            pltpu.SemaphoreType.REGULAR,
        ],
        compiler_params=pltpu.CompilerParams(
            collective_id=0, has_side_effects=True, vmem_limit_bytes=52 * 1024 * 1024
        ),
        cost_estimate=pl.CostEstimate(flops=4_000_000_000, bytes_accessed=8_000_000, transcendentals=0),
    )(*[pltpu.with_memory_space_constraint(x, pltpu.HBM) for x in operands])


def solution(mesh):
    return jax.shard_map(
        body,
        mesh=mesh,
        in_specs=(
            P("row", "grp", None, None, None),
            P("row", "grp", None),
            P("row", None, None, None),
            P(),
            P(),
        ),
        out_specs=P("row", "grp", None, None),
        check_vma=False,
    )
```

```python
import jax
import jax.numpy as jnp
from jax import lax
from jax.experimental import pallas as pl
from jax.experimental.pallas import tpu as pltpu
from jax.sharding import PartitionSpec as P

MESH = pl.DeviceIdType.MESH
F32 = jnp.float32
BF16 = jnp.bfloat16
I32 = jnp.int32
PLACE, WHICH, TARGET, PAIR, COLUMN = 0, 32, 48, 64, 80
BEHIND = 3
BEHIND_FIRST = 7


def kernel(
    a_cols_hbm, p_cols_hbm, c_cols_hbm, a_hbm, p_hbm, out_v,
    a_own, a_far, p_own, p_turn, band, begun, spreadable, placed, window, outer, inner,
    from_outer, from_inner, center, gathered, terms, terms_in, sums, sums_in, p_cols_v, c_cols_v, far_cols_v, tab_v, tab, own_cols, far_cols,
    load_sem, a_send, a_recv, c_send, c_recv, p_send, p_recv, s_send, s_recv, g_send, g_recv, t_send, t_recv, gate,
):
    grp = lax.axis_index("grp")
    row = lax.axis_index("row")
    n_row = lax.axis_size("row")
    core = lax.rem(row, 2)
    half = lax.rem(grp, 2)

    def along_row(by):
        return (grp, lax.rem(row + by + n_row, n_row))

    def along_grp(by):
        return (lax.rem(grp + by, 4), row)

    partner = (jnp.where(core == 0, grp + 1 - 2 * half, 3 - grp), row)
    sibling = (grp, row + 1 - 2 * core)
    outside = along_row(2 * core - 1)

    def remote(src, dst, send, recv, device):
        return pltpu.make_async_remote_copy(
            src_ref=src, dst_ref=dst, send_sem=send, recv_sem=recv, device_id=device, device_id_type=MESH
        )

    load_p = pltpu.make_async_copy(p_hbm, p_own, load_sem.at[0])
    load_p_cols = pltpu.make_async_copy(p_cols_hbm, p_cols_v.at[:, pl.ds(128, 1024)], load_sem.at[1])
    load_c_cols = pltpu.make_async_copy(c_cols_hbm, c_cols_v.at[:, pl.ds(128, 512)], load_sem.at[2])
    load_a = pltpu.make_async_copy(a_hbm, a_own, load_sem.at[3])
    load_own_cols = pltpu.make_async_copy(a_cols_hbm, own_cols, load_sem.at[4])
    for load in (load_p, load_p_cols, load_c_cols, load_a, load_own_cols):
        load.start()

    place_z = lax.rem(row // 2, 16)
    below = row >= 2
    above = row < n_row - 2
    first = (place_z == 0) & below
    last = (place_z == 15) & above
    has_outer = jnp.where(core == 0, row, n_row - 1 - row) >= 2

    barrier = pltpu.get_barrier_semaphore()

    def signal(semaphore, peer):
        pl.semaphore_signal(semaphore, inc=1, device_id=peer, device_id_type=MESH)

    for by in (1, 2, 3):
        signal(barrier, along_grp(by))
    signal(barrier, sibling)

    @pl.when(below)
    def _():
        signal(barrier, along_row(-2))

    @pl.when(below & (core == 0))
    def _():
        signal(barrier, along_row(-1))

    @pl.when(above & jnp.logical_not(last))
    def _():
        signal(barrier, along_row(2))

    @pl.when(above & jnp.logical_not(last) & (core == 1))
    def _():
        signal(barrier, along_row(1))


    lane = lax.broadcasted_iota(I32, (1, 128), 1)

    def from_lane(ref, start):
        begin = start + 128
        tile = begin // 128
        shift = lax.rem(begin, 128)
        first = pltpu.roll(ref[:, pl.ds(pl.multiple_of(tile * 128, 128), 128)], 128 - shift, 1)
        second = pltpu.roll(ref[:, pl.ds(pl.multiple_of(tile * 128 + 128, 128), 128)], 128 - shift, 1)
        return jnp.where(lane < 128 - shift, first, second)

    left = lax.broadcasted_iota(I32, (128, 128), 1) < 64
    left16 = lax.broadcasted_iota(jnp.int16, (128, 128), 1) < 64

    def turn(x):
        return pltpu.roll(x.astype(F32), 64, 1).astype(x.dtype)

    def prepare():
        load_p_cols.wait()
        load_c_cols.wait()
        band_cols = from_lane(p_cols_v, row * 8 - 16)
        sub = lax.broadcasted_iota(I32, (32, 128), 0)
        place = jnp.full((32, 128), 4, I32)
        which = jnp.full((16, 128), 4, I32)
        pair = jnp.full((16, 128), 160, I32)
        for p in range(4):
            cols = band_cols[p : p + 1]
            column = cols - (row - 3) * 4
            place = jnp.where(column == sub, p, place)
            which = jnp.where(cols - (row - 1) * 4 == sub[:16], p, which)
            pair = jnp.where((column == 2 * sub[:16]) | (column == 2 * sub[:16] + 1), 4 * lane + p, pair)
        columns = jnp.clip(band_cols - (row - 3) * 4, 0, 27)
        target = from_lane(c_cols_v, row * 4 - 4) - (row - 3) * 4
        tab_v[PLACE : PLACE + 32] = place
        tab_v[PAIR : PAIR + 16] = pair
        tab_v[COLUMN : COLUMN + 4] = columns - (columns & 1)
        tab_v[WHICH : WHICH + 16] = which
        tab_v[TARGET : TARGET + 16] = jnp.where((target >= 0) & (target < 28), target, 28)

        load_p.wait()

        def halve(i, carry):
            for pair in range(2):
                x, y = p_own[i, 2 * pair], p_own[i, 2 * pair + 1]
                x_turned, y_turned = turn(x), turn(y)
                band[2, i, pair] = jnp.where(half == 0, jnp.where(left, x, y_turned), jnp.where(left, x_turned, y))
            return carry

        lax.fori_loop(0, 8, halve, 0)

    early = (grp < 2) | (place_z < 8)

    @pl.when(early)
    def _():
        prepare()

    pl.semaphore_wait(barrier, 4 + jnp.where(above, 1 + core, 0) + jnp.where(below & jnp.logical_not(first), 2 - core, 0))

    @pl.when(last & (core == 1))
    def _():
        signal(gate, along_row(1))

    @pl.when(last)
    def _():
        signal(gate, along_row(2))


    def a_copy(i):
        return remote(a_hbm.at[i], a_far.at[i], a_send.at[i], a_recv.at[i], partner)

    def last_copy(part):
        slots = pl.ds(5 * part, 5 - 3 * part)
        return remote(a_hbm.at[7, slots], a_far.at[7, slots], a_send.at[7 + part], a_recv.at[7 + part], partner)

    cols_copy = remote(a_cols_hbm, far_cols_v, c_send, c_recv, partner)
    cols_copy.start()
    for i in range(7):
        a_copy(i).start()
    for part in range(2):
        last_copy(part).start()

    @pl.when(jnp.logical_not(early))
    def _():
        prepare()

    near = 3 - 2 * core

    def p_copy(kind, src, dst, n, device):
        return remote(band.at[src, n], band.at[dst, n], p_send.at[kind, n], p_recv.at[dst, n], device)

    def p_next(n):
        return p_copy(0, 2, 0, n, along_row(2))

    def p_prev(n):
        return p_copy(1, 2, 4, n, along_row(-2))

    def p_sibling(n):
        return p_copy(2, 2, 4 - near, n, sibling)

    def p_pass(n):
        return p_copy(3, 4 - 4 * core, near, n, sibling)

    def start_all(copy):
        def one(n, carry):
            copy(n).start()
            return carry

        lax.fori_loop(0, 8, one, 0)

    @pl.when(above & (core == 1))
    def _():
        start_all(p_next)

    @pl.when(below & jnp.logical_not(first) & (core == 0))
    def _():
        start_all(p_prev)

    start_all(p_sibling)

    to_smem = pltpu.make_async_copy(tab_v, tab, load_sem.at[5])
    to_smem.start()

    def transpose(i, carry):
        for q in range(4):
            p_turn[i, q] = p_own[i, q].T
        p_turn[i, 4] = jnp.zeros((128, 128), BF16)
        window[i, 28] = jnp.zeros((128, 128), BF16)
        return carry

    lax.fori_loop(0, 8, transpose, 0)
    spreadable[4] = jnp.zeros((128, 128), BF16)
    placed[160] = jnp.zeros((128, 128), BF16)
    to_smem.wait()

    def place_lines(slot, begin, count):
        def one(n, carry):
            line = slot * 8 + n
            for pair in range(2):
                x = band[slot, n, pair]
                turned = turn(x)
                spreadable[2 * pair] = jnp.where(left16, x, turned)
                spreadable[2 * pair + 1] = jnp.where(left16, turned, x)
            for p in range(4):
                column = tab[COLUMN + p, line]
                before = spreadable[tab[PLACE + column, line]]
                after = spreadable[tab[PLACE + 1 + column, line]]
                placed[4 * line + p] = jnp.where(left16, before, after)
            return carry

        lax.fori_loop(begin, begin + count, one, 0)

    def arrived(slot, n):
        p_copy(0, slot, slot, n, sibling).wait_recv()

    def there(slot):
        return jnp.where(slot > 2, above, below)

    def take(slot, n):
        @pl.when(there(slot))
        def _():
            arrived(slot, n)

            @pl.when(slot == 4 - 4 * core)
            def _():
                p_pass(n).start()

            place_lines(slot, n, 1)

    def follow(slot, n):
        @pl.when((n >= 0) & (slot == 4 - near) & there(slot))
        def _():
            arrived(slot, n)
            place_lines(slot, n, 1)

    place_lines(2, 0, 8)
    for n in range(8):
        arrived(near, n)
    place_lines(near, 0, 8)

    cols_copy.wait_recv()
    far_to_smem = pltpu.make_async_copy(far_cols_v, far_cols, load_sem.at[6])
    far_to_smem.start()
    load_own_cols.wait()
    load_a.wait()
    far_to_smem.wait()
    first_line = row * 8 - 16

    def tile_maker(i, slots):
        lhs = jnp.concatenate([(a_own if s < 7 else a_far)[i, s % 7] for s in slots], axis=1)
        lines = [(own_cols if s < 7 else far_cols)[s % 7, 0, i] - first_line for s in slots]
        lines = [jnp.clip(line, 0, 39) for line in lines]

        def tile(n):
            rhs = jnp.concatenate(
                [
                    jnp.concatenate([placed[tab[PAIR + 2 * n + u, line]] for line in lines], axis=0)
                    for u in range(2)
                ],
                axis=1,
            )
            return jnp.dot(lhs, rhs, preferred_element_type=F32)

        return tile

    def split(i, n, acc):
        for u in range(2):
            value = acc[:, u * 128 : (u + 1) * 128]
            high = value.astype(BF16).astype(F32)
            low = value - high
            window[i, 4 * n + 2 * u] = jnp.where(left, high, pltpu.roll(low, 64, 1)).astype(BF16)
            window[i, 4 * n + 2 * u + 1] = jnp.where(left, pltpu.roll(high, 64, 1), low).astype(BF16)

    def fine_row(i, begin, count):
        tile = tile_maker(i, range(14))
        for n in [begin + k for k in range(count)]:
            split(i, n, tile(n))

    def last_row():
        last_copy(0).wait_recv()
        tile = tile_maker(7, range(12))
        for n in range(7):
            begun[n] = tile(n)
        last_copy(1).wait_recv()
        tile = tile_maker(7, range(12, 14))
        for n in range(7):
            split(7, n, begun[n] + tile(n))

    ahead = first & (core == 0)
    late_near = last & (core == 0)
    late_follow = last & (core == 1)
    late_take = first & (core == 1)

    def follow_all(n, carry):
        follow(4 - near, n)

        @pl.when((n == 1) & late_near)
        def _():
            start_all(p_next)

        return carry

    def take_near(n, carry):
        take(4 - 4 * core, n)

        @pl.when(jnp.logical_not(ahead | last))
        def _():
            follow(4 - near, n - 2)

        @pl.when(late_take)
        def _():
            take(4 * core, n)

        @pl.when((n == 5) & above & (core == 0) & jnp.logical_not(last))
        def _():
            start_all(p_next)

        @pl.when((n == jnp.where(first, 3, 5)) & below & (core == 1))
        def _():
            @pl.when(first)
            def _():
                pl.semaphore_wait(gate, 1)

            start_all(p_prev)

        return carry

    def take_far(n, carry):
        take(4 * core, n)
        return carry

    def four_tiles(i, carry):
        a_copy(2 * i).wait_recv()
        a_copy(2 * i + 1).wait_recv()
        fine_row(2 * i, 3 - 3 * core, 4)
        fine_row(2 * i + 1, 3 - 3 * core, 4)
        return carry

    def other_three_tiles(i, carry):
        fine_row(2 * i, 4 * core, 3)
        fine_row(2 * i + 1, 4 * core, 3)
        return carry

    def three_tiles(i, carry):
        a_copy(2 * i).wait_recv()
        a_copy(2 * i + 1).wait_recv()
        fine_row(2 * i, 0, 3)
        fine_row(2 * i + 1, 0, 3)
        return carry

    def other_four_tiles(i, carry):
        fine_row(2 * i, 3, 4)
        fine_row(2 * i + 1, 3, 4)
        return carry

    def two_rows(i, carry):
        a_copy(2 * i).wait_recv()
        a_copy(2 * i + 1).wait_recv()
        fine_row(2 * i, 0, 7)
        fine_row(2 * i + 1, 0, 7)
        return carry

    def whole_row(i, carry):
        a_copy(i).wait_recv()
        fine_row(i, 0, 7)
        return carry

    @pl.when(late_near)
    def _():
        lax.fori_loop(0, 8, follow_all, 0)

    lax.fori_loop(0, 8, take_near, 0)

    @pl.when(ahead)
    def _():
        pl.semaphore_wait(gate, 2)
        start_all(p_prev)
        lax.fori_loop(0, 8, follow_all, 0)

    @pl.when(jnp.logical_not(ahead | last))
    def _():
        follow(4 - near, 6)
        follow(4 - near, 7)

    pairs = jnp.where(ahead, 3, 2)

    @pl.when(late_follow)
    def _():
        lax.fori_loop(0, 2, three_tiles, 0)
        lax.fori_loop(0, 8, follow_all, 0)
        lax.fori_loop(0, 8, take_far, 0)
        lax.fori_loop(0, 2, other_four_tiles, 0)

    @pl.when(jnp.logical_not(late_follow))
    def _():
        lax.fori_loop(0, pairs, four_tiles, 0)
        lax.fori_loop(jnp.where(late_take, 8, 0), 8, take_far, 0)
        lax.fori_loop(0, pairs, other_three_tiles, 0)

    lax.fori_loop(pairs, 3, two_rows, 0)

    whole_row(6, 0)

    @pl.when(jnp.logical_not(last))
    def _():
        last_row()

    @pl.when(last)
    def _():
        last_copy(0).wait_recv()
        last_copy(1).wait_recv()
        fine_row(7, 0, 7)

    def unit(n):
        early = n < 12
        return jnp.where(early, n // 3, n - 12), jnp.where(early, lax.rem(n, 3), 3)

    def steps(t):
        return jnp.where(t == 0, 2, jnp.where(t == 1, 1, jnp.where(t == 2, 3, 0)))

    def coarse_tiles(c, t):
        lhs = jnp.concatenate([p_turn[i, tab[WHICH + c, 16 + i]] for i in range(8)], axis=1)
        k = TARGET + lax.rem(grp + steps(t), 4) * 4
        tiles = []
        for pair in range(2):
            first = tab[k + 2 * pair, c]
            second = tab[k + 2 * pair + 1, c]
            rhs = jnp.concatenate(
                [jnp.concatenate([window[i, first], window[i, second]], axis=1) for i in range(8)], axis=0
            )
            acc = jnp.dot(lhs, rhs, preferred_element_type=F32)
            x, y = acc[:, :128], acc[:, 128:]
            tiles.append(jnp.where(left, x, y) + pltpu.roll(jnp.where(left, y, x), 64, 1))
        return tiles

    def outer_copy(n):
        return remote(outer.at[n], from_outer.at[n], s_send.at[0, n], s_recv.at[0, n], outside)

    sums_first = last & (core == 1)
    gets_sums = first & (core == 0)

    def by_sums(n):
        return unit(n)[0] == 0

    def sends_outer(n):
        return has_outer & jnp.logical_not(sums_first & by_sums(n))

    def gets_outer(n):
        return has_outer & jnp.logical_not(gets_sums & by_sums(n))

    def term_copy(t):
        return remote(terms.at[t], terms_in.at[t], t_send.at[t], t_recv.at[t], along_grp(steps(t)))

    def sums_copy():
        return remote(sums, sums_in, t_send.at[3], t_recv.at[3], outside)

    def whole_tiles(own, from_two, from_one, from_three):
        same = own + from_two
        other = from_one + from_three
        x = jnp.where(half == 0, same, other)
        y = jnp.where(half == 0, other, same)
        return jnp.where(left, x, pltpu.roll(y, 64, 1)), jnp.where(left, pltpu.roll(x, 64, 1), y)

    def inner_copy(n):
        return remote(inner.at[n], from_inner.at[n], s_send.at[1, n], s_recv.at[1, n], sibling)

    def group_copy(c, t):
        return remote(
            center.at[3 * c + t], gathered.at[t, c], g_send.at[t, c], g_recv.at[t, c], along_grp(steps(t))
        )

    def fill(ref, n, c, t):
        for pair, tile in enumerate(coarse_tiles(c, t)):
            ref[n, pair] = tile

    def absorb(n):
        inner_copy(n).wait_recv()

        @pl.when(gets_outer(n))
        def _():
            outer_copy(n).wait_recv()

        center[n] = center[n] + (from_inner[n] + jnp.where(gets_outer(n), from_outer[n], 0.0))

    behind = jnp.where(first & (core == 0), BEHIND_FIRST, jnp.where(last & (core == 1), BEHIND + 2, BEHIND))

    def sum_first(n):
        @pl.when(n < 4)
        def _():
            fill(terms, n, 8, n)

        @pl.when((n > 0) & (n < 4))
        def _():
            term_copy(n - 1).start()

        @pl.when(n == 8)
        def _():
            for t in range(3):
                term_copy(t).wait_recv()
            for pair in range(2):
                tiles = whole_tiles(terms[3, pair], terms_in[0, pair], terms_in[1, pair], terms_in[2, pair])
                sums[2 * pair], sums[2 * pair + 1] = tiles

        @pl.when(n == 12)
        def _():
            sums_copy().start()

    def one_unit(n, carry):
        c, t = unit(n)

        soon = gets_sums & (n >= 2) & (n < 5)
        done = jnp.where(soon, n - 2, n - behind)
        taken = (n >= behind + jnp.where(gets_sums, 3, 0)) | soon

        @pl.when(taken)
        def _():
            absorb(done)

        m = jnp.where(sums_first, jnp.where(n < 9, n + 3, jnp.where(n < 12, n + 4, 0)), n)
        outer_c, outer_t = unit(m)
        fill(outer, m, outer_c + 8 * core, outer_t)

        @pl.when(taken & (done < 12))
        def _():
            done_c, done_t = unit(done)
            group_copy(done_c, done_t).start()

        @pl.when(has_outer & jnp.logical_not(sums_first & (n >= 12)))
        def _():
            outer_copy(m).start()

        fill(inner, n, c + 8 - 8 * core, t)
        inner_copy(n).start()
        fill(center, n, c + 4, t)

        @pl.when(sums_first)
        def _():
            sum_first(n)

        return carry

    lax.fori_loop(0, 16, one_unit, 0)

    cols_copy.wait_send()
    for i in range(7):
        a_copy(i).wait_send()
    for part in range(2):
        last_copy(part).wait_send()
    for n in range(8):
        p_sibling(n).wait_send()

        @pl.when(above)
        def _():
            p_next(n).wait_send()

        @pl.when(below)
        def _():
            p_prev(n).wait_send()

        @pl.when(there(4 - 4 * core))
        def _():
            p_pass(n).wait_send()

    def finish(c):
        for t in range(3):
            group_copy(c, t).wait_recv()
        for pair in range(2):
            tiles = whole_tiles(
                center[12 + c, pair], gathered[0, c, pair], gathered[1, c, pair], gathered[2, c, pair]
            )
            out_v[c, 2 * pair], out_v[c, 2 * pair + 1] = tiles

    def absorb_rest(n, carry):
        absorb(n)

        @pl.when((n > 16 - behind) & (n < 13))
        def _():
            done_c, done_t = unit(n - 1)
            group_copy(done_c, done_t).start()

        @pl.when(n >= 13)
        def _():
            finish(n - 13)

        return carry

    lax.fori_loop(16 - behind, 15, absorb_rest, 0)
    finish(2)

    def sent(n, carry):
        inner_copy(n).wait_send()

        @pl.when(sends_outer(n))
        def _():
            outer_copy(n).wait_send()

        @pl.when(n < 9)
        def _():
            group_copy(n // 3, lax.rem(n, 3)).wait_send()

        return carry

    lax.fori_loop(0, 15, sent, 0)
    @pl.when(gets_sums)
    def _():
        sums_copy().wait_recv()
        out_v[0] = out_v[0] + sums_in[...]

    absorb(15)
    finish(3)

    @pl.when(sums_first)
    def _():
        for t in range(3):
            term_copy(t).wait_send()
        sums_copy().wait_send()

    sent(15, 0)
    for t in range(3):
        group_copy(3, t).wait_send()


def body(a_tiles, a_cols, p_tiles, p_cols, c_cols):
    operands = (a_cols.transpose(2, 1, 0), p_cols.T, c_cols.T, a_tiles.reshape(8, 7, 128, 128), p_tiles)
    dma = pltpu.SemaphoreType.DMA
    anywhere = pl.BlockSpec(memory_space=pl.ANY)
    side = pltpu.VMEM((16, 2, 128, 128), F32)
    return pl.pallas_call(
        kernel,
        out_shape=pltpu.VMEM((4, 4, 128, 128), F32),
        in_specs=[anywhere] * 5,
        out_specs=pl.BlockSpec(memory_space=pltpu.VMEM),
        scratch_shapes=[
            pltpu.VMEM((8, 7, 128, 128), BF16),
            pltpu.VMEM((8, 7, 128, 128), BF16),
            pltpu.VMEM((8, 4, 128, 128), BF16),
            pltpu.VMEM((8, 5, 128, 128), BF16),
            pltpu.VMEM((5, 8, 2, 128, 128), BF16),
            pltpu.VMEM((7, 128, 256), F32),
            pltpu.VMEM((5, 128, 128), BF16),
            pltpu.VMEM((161, 128, 128), BF16),
            pltpu.VMEM((8, 29, 128, 128), BF16),
            side,
            side,
            side,
            side,
            side,
            pltpu.VMEM((3, 4, 2, 128, 128), F32),
            pltpu.VMEM((4, 2, 128, 128), F32),
            pltpu.VMEM((3, 2, 128, 128), F32),
            pltpu.VMEM((4, 128, 128), F32),
            pltpu.VMEM((4, 128, 128), F32),
            pltpu.VMEM((4, 1280), I32),
            pltpu.VMEM((16, 768), I32),
            pltpu.VMEM((7, 1, 8), I32),
            pltpu.VMEM((88, 128), I32),
            pltpu.SMEM((88, 128), I32),
            pltpu.SMEM((7, 1, 8), I32),
            pltpu.SMEM((7, 1, 8), I32),
            dma((7,)),
            dma((9,)),
            dma((9,)),
            dma,
            dma,
            dma((4, 8)),
            dma((5, 8)),
            dma((2, 16)),
            dma((2, 16)),
            dma((3, 4)),
            dma((3, 4)),
            dma((4,)),
            dma((4,)),
            pltpu.SemaphoreType.REGULAR,
        ],
        compiler_params=pltpu.CompilerParams(
            collective_id=0, has_side_effects=True, vmem_limit_bytes=52 * 1024 * 1024
        ),
        cost_estimate=pl.CostEstimate(flops=4_000_000_000, bytes_accessed=8_000_000, transcendentals=0),
    )(*[pltpu.with_memory_space_constraint(x, pltpu.HBM) for x in operands])


def solution(mesh):
    return jax.shard_map(
        body,
        mesh=mesh,
        in_specs=(
            P("row", "grp", None, None, None),
            P("row", "grp", None),
            P("row", None, None, None),
            P(),
            P(),
        ),
        out_specs=P("row", "grp", None, None),
        check_vma=False,
    )
```

```python
import jax
import jax.numpy as jnp
from jax import lax
from jax.experimental import pallas as pl
from jax.experimental.pallas import tpu as pltpu
from jax.sharding import PartitionSpec as P

MESH = pl.DeviceIdType.MESH
F32 = jnp.float32
BF16 = jnp.bfloat16
I32 = jnp.int32
PLACE, WHICH, TARGET, PAIR, COLUMN = 0, 32, 48, 64, 80
BEHIND = 3
BEHIND_FIRST = 7


def kernel(
    a_cols_hbm, p_cols_hbm, c_cols_hbm, a_hbm, p_hbm, out_v,
    a_own, a_far, p_own, p_turn, band, begun, spreadable, placed, window, outer, inner,
    from_outer, from_inner, center, gathered, terms, terms_in, sums, sums_in, p_cols_v, c_cols_v, far_cols_v, tab_v, tab, own_cols, far_cols,
    load_sem, a_send, a_recv, c_send, c_recv, p_send, p_recv, s_send, s_recv, g_send, g_recv, t_send, t_recv, gate,
):
    grp = lax.axis_index("grp")
    row = lax.axis_index("row")
    n_row = lax.axis_size("row")
    core = lax.rem(row, 2)
    half = lax.rem(grp, 2)

    def along_row(by):
        return (grp, lax.rem(row + by + n_row, n_row))

    def along_grp(by):
        return (lax.rem(grp + by, 4), row)

    partner = (jnp.where(core == 0, grp + 1 - 2 * half, 3 - grp), row)
    sibling = (grp, row + 1 - 2 * core)
    outside = along_row(2 * core - 1)

    def remote(src, dst, send, recv, device):
        return pltpu.make_async_remote_copy(
            src_ref=src, dst_ref=dst, send_sem=send, recv_sem=recv, device_id=device, device_id_type=MESH
        )

    load_p = pltpu.make_async_copy(p_hbm, p_own, load_sem.at[0])
    load_p_cols = pltpu.make_async_copy(p_cols_hbm, p_cols_v.at[:, pl.ds(128, 1024)], load_sem.at[1])
    load_c_cols = pltpu.make_async_copy(c_cols_hbm, c_cols_v.at[:, pl.ds(128, 512)], load_sem.at[2])
    load_a = pltpu.make_async_copy(a_hbm, a_own, load_sem.at[3])
    load_own_cols = pltpu.make_async_copy(a_cols_hbm, own_cols, load_sem.at[4])
    for load in (load_p, load_p_cols, load_c_cols, load_a, load_own_cols):
        load.start()

    place_z = lax.rem(row // 2, 16)
    below = row >= 2
    above = row < n_row - 2
    first = (place_z == 0) & below
    last = (place_z == 15) & above
    has_outer = jnp.where(core == 0, row, n_row - 1 - row) >= 2

    barrier = pltpu.get_barrier_semaphore()

    def signal(semaphore, peer):
        pl.semaphore_signal(semaphore, inc=1, device_id=peer, device_id_type=MESH)

    for by in (1, 2, 3):
        signal(barrier, along_grp(by))
    signal(barrier, sibling)

    @pl.when(below)
    def _():
        signal(barrier, along_row(-2))

    @pl.when(below & (core == 0))
    def _():
        signal(barrier, along_row(-1))

    @pl.when(above & jnp.logical_not(last))
    def _():
        signal(barrier, along_row(2))

    @pl.when(above & jnp.logical_not(last) & (core == 1))
    def _():
        signal(barrier, along_row(1))


    lane = lax.broadcasted_iota(I32, (1, 128), 1)

    def from_lane(ref, start):
        begin = start + 128
        tile = begin // 128
        shift = lax.rem(begin, 128)
        first = pltpu.roll(ref[:, pl.ds(pl.multiple_of(tile * 128, 128), 128)], 128 - shift, 1)
        second = pltpu.roll(ref[:, pl.ds(pl.multiple_of(tile * 128 + 128, 128), 128)], 128 - shift, 1)
        return jnp.where(lane < 128 - shift, first, second)

    left = lax.broadcasted_iota(I32, (128, 128), 1) < 64
    left16 = lax.broadcasted_iota(jnp.int16, (128, 128), 1) < 64

    def turn(x):
        return pltpu.roll(x.astype(F32), 64, 1).astype(x.dtype)

    def prepare():
        load_p_cols.wait()
        load_c_cols.wait()
        band_cols = from_lane(p_cols_v, row * 8 - 16)
        sub = lax.broadcasted_iota(I32, (32, 128), 0)
        place = jnp.full((32, 128), 4, I32)
        which = jnp.full((16, 128), 4, I32)
        pair = jnp.full((16, 128), 160, I32)
        for p in range(4):
            cols = band_cols[p : p + 1]
            column = cols - (row - 3) * 4
            place = jnp.where(column == sub, p, place)
            which = jnp.where(cols - (row - 1) * 4 == sub[:16], p, which)
            pair = jnp.where((column == 2 * sub[:16]) | (column == 2 * sub[:16] + 1), 4 * lane + p, pair)
        columns = jnp.clip(band_cols - (row - 3) * 4, 0, 27)
        target = from_lane(c_cols_v, row * 4 - 4) - (row - 3) * 4
        tab_v[PLACE : PLACE + 32] = place
        tab_v[PAIR : PAIR + 16] = pair
        tab_v[COLUMN : COLUMN + 4] = columns - (columns & 1)
        tab_v[WHICH : WHICH + 16] = which
        tab_v[TARGET : TARGET + 16] = jnp.where((target >= 0) & (target < 28), target, 28)

        load_p.wait()

        def halve(i, carry):
            for pair in range(2):
                x, y = p_own[i, 2 * pair], p_own[i, 2 * pair + 1]
                x_turned, y_turned = turn(x), turn(y)
                band[2, i, pair] = jnp.where(half == 0, jnp.where(left, x, y_turned), jnp.where(left, x_turned, y))
            return carry

        lax.fori_loop(0, 8, halve, 0)

    early = (grp < 2) | (place_z < 8)

    @pl.when(early)
    def _():
        prepare()

    pl.semaphore_wait(barrier, 4 + jnp.where(above, 1 + core, 0) + jnp.where(below & jnp.logical_not(first), 2 - core, 0))

    @pl.when(last & (core == 1))
    def _():
        signal(gate, along_row(1))

    @pl.when(last)
    def _():
        signal(gate, along_row(2))


    def a_copy(i):
        return remote(a_hbm.at[i], a_far.at[i], a_send.at[i], a_recv.at[i], partner)

    def last_copy(part):
        slots = pl.ds(5 * part, 5 - 3 * part)
        return remote(a_hbm.at[7, slots], a_far.at[7, slots], a_send.at[7 + part], a_recv.at[7 + part], partner)

    cols_copy = remote(a_cols_hbm, far_cols_v, c_send, c_recv, partner)
    cols_copy.start()
    for i in range(7):
        a_copy(i).start()
    for part in range(2):
        last_copy(part).start()

    @pl.when(jnp.logical_not(early))
    def _():
        prepare()

    near = 3 - 2 * core

    def p_copy(kind, src, dst, n, device):
        return remote(band.at[src, n], band.at[dst, n], p_send.at[kind, n], p_recv.at[dst, n], device)

    def p_next(n):
        return p_copy(0, 2, 0, n, along_row(2))

    def p_prev(n):
        return p_copy(1, 2, 4, n, along_row(-2))

    def p_sibling(n):
        return p_copy(2, 2, 4 - near, n, sibling)

    def p_pass(n):
        return p_copy(3, 4 - 4 * core, near, n, sibling)

    def start_all(copy):
        def one(n, carry):
            copy(n).start()
            return carry

        lax.fori_loop(0, 8, one, 0)

    @pl.when(above & (core == 1))
    def _():
        start_all(p_next)

    @pl.when(below & jnp.logical_not(first) & (core == 0))
    def _():
        start_all(p_prev)

    start_all(p_sibling)

    to_smem = pltpu.make_async_copy(tab_v, tab, load_sem.at[5])
    to_smem.start()

    def transpose(i, carry):
        for q in range(4):
            p_turn[i, q] = p_own[i, q].T
        p_turn[i, 4] = jnp.zeros((128, 128), BF16)
        window[i, 28] = jnp.zeros((128, 128), BF16)
        return carry

    lax.fori_loop(0, 8, transpose, 0)
    spreadable[4] = jnp.zeros((128, 128), BF16)
    placed[160] = jnp.zeros((128, 128), BF16)
    to_smem.wait()

    def place_lines(slot, begin, count):
        def one(n, carry):
            line = slot * 8 + n
            for pair in range(2):
                x = band[slot, n, pair]
                turned = turn(x)
                spreadable[2 * pair] = jnp.where(left16, x, turned)
                spreadable[2 * pair + 1] = jnp.where(left16, turned, x)
            for p in range(4):
                column = tab[COLUMN + p, line]
                before = spreadable[tab[PLACE + column, line]]
                after = spreadable[tab[PLACE + 1 + column, line]]
                placed[4 * line + p] = jnp.where(left16, before, after)
            return carry

        lax.fori_loop(begin, begin + count, one, 0)

    def arrived(slot, n):
        p_copy(0, slot, slot, n, sibling).wait_recv()

    def there(slot):
        return jnp.where(slot > 2, above, below)

    def take(slot, n):
        @pl.when(there(slot))
        def _():
            arrived(slot, n)

            @pl.when(slot == 4 - 4 * core)
            def _():
                p_pass(n).start()

            place_lines(slot, n, 1)

    def follow(slot, n):
        @pl.when((n >= 0) & (slot == 4 - near) & there(slot))
        def _():
            arrived(slot, n)
            place_lines(slot, n, 1)

    place_lines(2, 0, 8)
    for n in range(8):
        arrived(near, n)
    place_lines(near, 0, 8)

    cols_copy.wait_recv()
    far_to_smem = pltpu.make_async_copy(far_cols_v, far_cols, load_sem.at[6])
    far_to_smem.start()
    load_own_cols.wait()
    load_a.wait()
    far_to_smem.wait()
    first_line = row * 8 - 16

    def tile_maker(i, slots):
        lhs = jnp.concatenate([(a_own if s < 7 else a_far)[i, s % 7] for s in slots], axis=1)
        lines = [(own_cols if s < 7 else far_cols)[s % 7, 0, i] - first_line for s in slots]
        lines = [jnp.clip(line, 0, 39) for line in lines]

        def tile(n):
            rhs = jnp.concatenate(
                [
                    jnp.concatenate([placed[tab[PAIR + 2 * n + u, line]] for line in lines], axis=0)
                    for u in range(2)
                ],
                axis=1,
            )
            return jnp.dot(lhs, rhs, preferred_element_type=F32)

        return tile

    def split(i, n, acc):
        for u in range(2):
            value = acc[:, u * 128 : (u + 1) * 128]
            high = value.astype(BF16).astype(F32)
            low = value - high
            window[i, 4 * n + 2 * u] = jnp.where(left, high, pltpu.roll(low, 64, 1)).astype(BF16)
            window[i, 4 * n + 2 * u + 1] = jnp.where(left, pltpu.roll(high, 64, 1), low).astype(BF16)

    def fine_row(i, begin, count):
        tile = tile_maker(i, range(14))
        for n in [begin + k for k in range(count)]:
            split(i, n, tile(n))

    def last_row():
        last_copy(0).wait_recv()
        tile = tile_maker(7, range(12))
        for n in range(7):
            begun[n] = tile(n)
        last_copy(1).wait_recv()
        tile = tile_maker(7, range(12, 14))
        for n in range(7):
            split(7, n, begun[n] + tile(n))

    ahead = first & (core == 0)
    late_near = last & (core == 0)
    late_follow = last & (core == 1)
    late_take = first & (core == 1)

    def follow_all(n, carry):
        follow(4 - near, n)

        @pl.when((n == 1) & late_near)
        def _():
            start_all(p_next)

        return carry

    def take_near(n, carry):
        take(4 - 4 * core, n)

        @pl.when(jnp.logical_not(ahead | last))
        def _():
            follow(4 - near, n - 2)

        @pl.when(late_take)
        def _():
            take(4 * core, n)

        @pl.when((n == 5) & above & (core == 0) & jnp.logical_not(last))
        def _():
            start_all(p_next)

        @pl.when((n == jnp.where(first, 3, 5)) & below & (core == 1))
        def _():
            @pl.when(first)
            def _():
                pl.semaphore_wait(gate, 1)

            start_all(p_prev)

        return carry

    def take_far(n, carry):
        take(4 * core, n)
        return carry

    def four_tiles(i, carry):
        a_copy(2 * i).wait_recv()
        a_copy(2 * i + 1).wait_recv()
        fine_row(2 * i, 3 - 3 * core, 4)
        fine_row(2 * i + 1, 3 - 3 * core, 4)
        return carry

    def other_three_tiles(i, carry):
        fine_row(2 * i, 4 * core, 3)
        fine_row(2 * i + 1, 4 * core, 3)
        return carry

    def three_tiles(i, carry):
        a_copy(2 * i).wait_recv()
        a_copy(2 * i + 1).wait_recv()
        fine_row(2 * i, 0, 3)
        fine_row(2 * i + 1, 0, 3)
        return carry

    def other_four_tiles(i, carry):
        fine_row(2 * i, 3, 4)
        fine_row(2 * i + 1, 3, 4)
        return carry

    def two_rows(i, carry):
        a_copy(2 * i).wait_recv()
        a_copy(2 * i + 1).wait_recv()
        fine_row(2 * i, 0, 7)
        fine_row(2 * i + 1, 0, 7)
        return carry

    def whole_row(i, carry):
        a_copy(i).wait_recv()
        fine_row(i, 0, 7)
        return carry

    @pl.when(late_near)
    def _():
        lax.fori_loop(0, 8, follow_all, 0)

    lax.fori_loop(0, 8, take_near, 0)

    @pl.when(ahead)
    def _():
        pl.semaphore_wait(gate, 2)
        start_all(p_prev)
        lax.fori_loop(0, 8, follow_all, 0)

    @pl.when(jnp.logical_not(ahead | last))
    def _():
        follow(4 - near, 6)
        follow(4 - near, 7)

    pairs = jnp.where(ahead, 3, 2)

    @pl.when(late_follow)
    def _():
        lax.fori_loop(0, 2, three_tiles, 0)
        lax.fori_loop(0, 8, follow_all, 0)
        lax.fori_loop(0, 8, take_far, 0)
        lax.fori_loop(0, 2, other_four_tiles, 0)

    @pl.when(jnp.logical_not(late_follow))
    def _():
        lax.fori_loop(0, pairs, four_tiles, 0)
        lax.fori_loop(jnp.where(late_take, 8, 0), 8, take_far, 0)
        lax.fori_loop(0, pairs, other_three_tiles, 0)

    lax.fori_loop(pairs, 3, two_rows, 0)

    whole_row(6, 0)

    @pl.when(jnp.logical_not(last))
    def _():
        last_row()

    @pl.when(last)
    def _():
        last_copy(0).wait_recv()
        last_copy(1).wait_recv()
        fine_row(7, 0, 7)

    def unit(n):
        early = n < 12
        return jnp.where(early, n // 3, n - 12), jnp.where(early, lax.rem(n, 3), 3)

    def steps(t):
        return jnp.where(t == 0, 2, jnp.where(t == 1, 1, jnp.where(t == 2, 3, 0)))

    def coarse_tiles(c, t):
        lhs = jnp.concatenate([p_turn[i, tab[WHICH + c, 16 + i]] for i in range(8)], axis=1)
        k = TARGET + lax.rem(grp + steps(t), 4) * 4
        tiles = []
        for pair in range(2):
            first = tab[k + 2 * pair, c]
            second = tab[k + 2 * pair + 1, c]
            rhs = jnp.concatenate(
                [jnp.concatenate([window[i, first], window[i, second]], axis=1) for i in range(8)], axis=0
            )
            acc = jnp.dot(lhs, rhs, preferred_element_type=F32)
            x, y = acc[:, :128], acc[:, 128:]
            tiles.append(jnp.where(left, x, y) + pltpu.roll(jnp.where(left, y, x), 64, 1))
        return tiles

    def outer_copy(n):
        return remote(outer.at[n], from_outer.at[n], s_send.at[0, n], s_recv.at[0, n], outside)

    sums_first = last & (core == 1)
    gets_sums = first & (core == 0)

    def by_sums(n):
        return unit(n)[0] == 0

    def sends_outer(n):
        return has_outer & jnp.logical_not(sums_first & by_sums(n))

    def gets_outer(n):
        return has_outer & jnp.logical_not(gets_sums & by_sums(n))

    def term_copy(t):
        return remote(terms.at[t], terms_in.at[t], t_send.at[t], t_recv.at[t], along_grp(steps(t)))

    def sums_copy():
        return remote(sums, sums_in, t_send.at[3], t_recv.at[3], outside)

    def whole_tiles(own, from_two, from_one, from_three):
        same = own + from_two
        other = from_one + from_three
        x = jnp.where(half == 0, same, other)
        y = jnp.where(half == 0, other, same)
        return jnp.where(left, x, pltpu.roll(y, 64, 1)), jnp.where(left, pltpu.roll(x, 64, 1), y)

    def inner_copy(n):
        return remote(inner.at[n], from_inner.at[n], s_send.at[1, n], s_recv.at[1, n], sibling)

    def group_copy(c, t):
        return remote(
            center.at[3 * c + t], gathered.at[t, c], g_send.at[t, c], g_recv.at[t, c], along_grp(steps(t))
        )

    def fill(ref, n, c, t):
        for pair, tile in enumerate(coarse_tiles(c, t)):
            ref[n, pair] = tile

    def absorb(n):
        inner_copy(n).wait_recv()

        @pl.when(gets_outer(n))
        def _():
            outer_copy(n).wait_recv()

        center[n] = center[n] + (from_inner[n] + jnp.where(gets_outer(n), from_outer[n], 0.0))

    behind = jnp.where(first & (core == 0), BEHIND_FIRST, BEHIND)

    def sum_first(n):
        @pl.when(n < 4)
        def _():
            fill(terms, n, 8, n)

        @pl.when((n > 0) & (n < 4))
        def _():
            term_copy(n - 1).start()

        @pl.when(n == 8)
        def _():
            for t in range(3):
                term_copy(t).wait_recv()
            for pair in range(2):
                tiles = whole_tiles(terms[3, pair], terms_in[0, pair], terms_in[1, pair], terms_in[2, pair])
                sums[2 * pair], sums[2 * pair + 1] = tiles

        @pl.when(n == 12)
        def _():
            sums_copy().start()

    def one_unit(n, carry):
        c, t = unit(n)

        soon = gets_sums & (n >= 2) & (n < 5)
        done = jnp.where(soon, n - 2, n - behind)
        taken = (n >= behind + jnp.where(gets_sums, 3, 0)) | soon

        @pl.when(taken)
        def _():
            absorb(done)

        m = jnp.where(sums_first, jnp.where(n < 9, n + 3, jnp.where(n < 12, n + 4, 0)), n)
        outer_c, outer_t = unit(m)
        fill(outer, m, outer_c + 8 * core, outer_t)

        @pl.when(taken & (done < 12))
        def _():
            done_c, done_t = unit(done)
            group_copy(done_c, done_t).start()

        @pl.when(has_outer & jnp.logical_not(sums_first & (n >= 12)))
        def _():
            outer_copy(m).start()

        fill(inner, n, c + 8 - 8 * core, t)
        inner_copy(n).start()
        fill(center, n, c + 4, t)

        @pl.when(sums_first)
        def _():
            sum_first(n)

        return carry

    lax.fori_loop(0, 16, one_unit, 0)

    cols_copy.wait_send()
    for i in range(7):
        a_copy(i).wait_send()
    for part in range(2):
        last_copy(part).wait_send()
    for n in range(8):
        p_sibling(n).wait_send()

        @pl.when(above)
        def _():
            p_next(n).wait_send()

        @pl.when(below)
        def _():
            p_prev(n).wait_send()

        @pl.when(there(4 - 4 * core))
        def _():
            p_pass(n).wait_send()

    def finish(c):
        for t in range(3):
            group_copy(c, t).wait_recv()
        for pair in range(2):
            tiles = whole_tiles(
                center[12 + c, pair], gathered[0, c, pair], gathered[1, c, pair], gathered[2, c, pair]
            )
            out_v[c, 2 * pair], out_v[c, 2 * pair + 1] = tiles

    def absorb_rest(n, carry):
        absorb(n)

        @pl.when((n > 16 - behind) & (n < 13))
        def _():
            done_c, done_t = unit(n - 1)
            group_copy(done_c, done_t).start()

        @pl.when(n >= 13)
        def _():
            finish(n - 13)

        return carry

    lax.fori_loop(16 - behind, 15, absorb_rest, 0)
    finish(2)

    def sent(n, carry):
        inner_copy(n).wait_send()

        @pl.when(sends_outer(n))
        def _():
            outer_copy(n).wait_send()

        @pl.when(n < 9)
        def _():
            group_copy(n // 3, lax.rem(n, 3)).wait_send()

        return carry

    lax.fori_loop(0, 15, sent, 0)
    @pl.when(gets_sums)
    def _():
        sums_copy().wait_recv()
        out_v[0] = out_v[0] + sums_in[...]

    absorb(15)
    finish(3)

    @pl.when(sums_first)
    def _():
        for t in range(3):
            term_copy(t).wait_send()
        sums_copy().wait_send()

    sent(15, 0)
    for t in range(3):
        group_copy(3, t).wait_send()


def body(a_tiles, a_cols, p_tiles, p_cols, c_cols):
    operands = (a_cols.transpose(2, 1, 0), p_cols.T, c_cols.T, a_tiles.reshape(8, 7, 128, 128), p_tiles)
    dma = pltpu.SemaphoreType.DMA
    anywhere = pl.BlockSpec(memory_space=pl.ANY)
    side = pltpu.VMEM((16, 2, 128, 128), F32)
    return pl.pallas_call(
        kernel,
        out_shape=pltpu.VMEM((4, 4, 128, 128), F32),
        in_specs=[anywhere] * 5,
        out_specs=pl.BlockSpec(memory_space=pltpu.VMEM),
        scratch_shapes=[
            pltpu.VMEM((8, 7, 128, 128), BF16),
            pltpu.VMEM((8, 7, 128, 128), BF16),
            pltpu.VMEM((8, 4, 128, 128), BF16),
            pltpu.VMEM((8, 5, 128, 128), BF16),
            pltpu.VMEM((5, 8, 2, 128, 128), BF16),
            pltpu.VMEM((7, 128, 256), F32),
            pltpu.VMEM((5, 128, 128), BF16),
            pltpu.VMEM((161, 128, 128), BF16),
            pltpu.VMEM((8, 29, 128, 128), BF16),
            side,
            side,
            side,
            side,
            side,
            pltpu.VMEM((3, 4, 2, 128, 128), F32),
            pltpu.VMEM((4, 2, 128, 128), F32),
            pltpu.VMEM((3, 2, 128, 128), F32),
            pltpu.VMEM((4, 128, 128), F32),
            pltpu.VMEM((4, 128, 128), F32),
            pltpu.VMEM((4, 1280), I32),
            pltpu.VMEM((16, 768), I32),
            pltpu.VMEM((7, 1, 8), I32),
            pltpu.VMEM((88, 128), I32),
            pltpu.SMEM((88, 128), I32),
            pltpu.SMEM((7, 1, 8), I32),
            pltpu.SMEM((7, 1, 8), I32),
            dma((7,)),
            dma((9,)),
            dma((9,)),
            dma,
            dma,
            dma((4, 8)),
            dma((5, 8)),
            dma((2, 16)),
            dma((2, 16)),
            dma((3, 4)),
            dma((3, 4)),
            dma((4,)),
            dma((4,)),
            pltpu.SemaphoreType.REGULAR,
        ],
        compiler_params=pltpu.CompilerParams(
            collective_id=0, has_side_effects=True, vmem_limit_bytes=52 * 1024 * 1024
        ),
        cost_estimate=pl.CostEstimate(flops=4_000_000_000, bytes_accessed=8_000_000, transcendentals=0),
    )(*[pltpu.with_memory_space_constraint(x, pltpu.HBM) for x in operands])


def solution(mesh):
    return jax.shard_map(
        body,
        mesh=mesh,
        in_specs=(
            P("row", "grp", None, None, None),
            P("row", "grp", None),
            P("row", None, None, None),
            P(),
            P(),
        ),
        out_specs=P("row", "grp", None, None),
        check_vma=False,
    )
```
